32 devices in a mesh: dp: 8 (over z, x), mp: 4 (over y, core).
Axes of the slice: x: 2, y: 2, z: 4, core: 2. Of those that a mesh axis runs over, the one named last changes fastest.
Arguments:
- q_latent: bfloat16 [2048, 2, 768], P('dp', None, 'mp'), may hold values from -6 to 6
- kv_latent: bfloat16 [2048, 2, 256], P('dp', None, 'mp'), may hold values from -6 to 6
- q_head_grad: bfloat16 [2048, 512], P('dp'), may hold values from -0.1875 to 0.1875
- k_head_grad: bfloat16 [2048, 512], P('dp'), may hold values from -0.1875 to 0.1875
- q_heads: bfloat16 [2048, 512], P('dp', 'mp'), may hold values from -6 to 6
- k_heads: bfloat16 [2048, 512], P('dp', 'mp'), may hold values from -6 to 6
- query_pick: int32 [8, 16, 4], P('dp', None, 'mp'), may hold values from 0 to 255
- key_pick: int32 [8, 16, 4], P('dp', None, 'mp'), may hold values from 0 to 255
- q_weight: float32 [8, 768, 128], P('dp', 'mp'), may hold values from -6 to 6
- k_weight: float32 [8, 256, 128], P('dp', 'mp'), may hold values from -6 to 6
- q_moment: float32 [8, 768, 128], P('dp', 'mp'), may hold values from -6 to 6
- k_moment: float32 [8, 256, 128], P('dp', 'mp'), may hold values from -6 to 6
Outputs:
- q_weight_new: float32 [8, 768, 128], P('dp', 'mp')
- k_weight_new: float32 [8, 256, 128], P('dp', 'mp')
- q_moment_new: float32 [8, 768, 128], P('dp', 'mp')
- k_moment_new: float32 [8, 256, 128], P('dp', 'mp')
The draws below stay inside these ranges and needn't reach their ends.
Inputs may be any that keep to these rules, and one draw needn't show every extreme that they name: `query_pick`: the index of a token among the 256 tokens of its own block b. `key_pick`: the index of a token among the 256 tokens of its own block b.
All inputs are finite; a program needn't handle non-finite values.
Results may differ from the reference program's by a relative error of at most 0.0003.
Values sent between devices are 32-bit elements; how exact they have to be, the bound alone decides.
No kernel may reach another device: no remote copies, remote signals or barrier semaphores. Data moves between devices by JAX's collectives and lax.ppermute only.
A program may use at most 64 MiB of HBM per device.

```python
import math
import jax
import jax.numpy as jnp
from jax import lax

QR = 1536
KR = 512
DN = 128
TOK_DEV = 256
PICKS = 16
ITERS = 5
HEADS = 4
TOKENS = 2048
N_DP = 8


def touch_ends(result, stream_key, low, top_value):
    dims = result.shape
    spot = [jax.random.randint(jax.random.fold_in(stream_key, axis), (), 0, dims[axis]) for axis in range(len(dims))]
    result = result.at[tuple(spot)].set(low)
    longest = dims.index(max(dims))
    spot[longest] = (spot[longest] + 1) % dims[longest]
    return result.at[tuple(spot)].set(top_value)


def strengthened(result, stream_key, source, target, parts, factor):
    owner, partner = [(jnp.arange(result.shape[axis_at]) // (result.shape[axis_at] // parts)).reshape([-1 if axis == axis_at else 1 for axis in range(result.ndim)]) for axis_at in (source, target)]
    chosen = jax.random.permutation(stream_key, parts)[partner]
    strong = (owner == chosen) | (owner == (partner + parts // 2) % parts)
    return jnp.where(strong, factor * result, result)


def levels(key, dims, pieces, low, high):
    def one(position, shards_of):
        steps = jax.random.uniform(jax.random.fold_in(jax.random.fold_in(key, 6), position), (shards_of,), jnp.float32, low / len(pieces), high / len(pieces))
        return jnp.repeat(jnp.exp(steps), dims[position] // shards_of).reshape((-1,) + (1,) * (len(dims) - position - 1))

    loudness = one(*pieces[0])
    for cut in pieces[1:]:
        loudness = loudness * one(*cut)
    return loudness


def gaussian(own_key, extent, spread, bound, cuts=(), kind=jnp.bfloat16):
    result = spread * jax.random.normal(own_key, extent, jnp.float32)
    if cuts:
        result = result * levels(own_key, extent, cuts, -0.22, 0.18)
    return jnp.clip(result, -bound, bound).astype(kind)


def bell_draw_with(rng, dims, scale, limit, shards, heavy, held_as=jnp.bfloat16):
    entries = scale * jax.random.normal(rng, dims, jnp.float32)
    if shards:
        entries = entries * levels(rng, dims, shards, -0.22, 0.18)
    return jnp.clip(strengthened(entries, jax.random.fold_in(rng, 3), *heavy), -limit, limit).astype(held_as)


def setup_inputs(seed: int = 0) -> dict:
    key_list = jax.random.split(jax.random.key(seed), 13)
    return {
        "q_latent": gaussian(key_list[0], (TOKENS, 2, QR // 2), 1.0, 6.0, ((0, 8), (2, 4))),
        "kv_latent": gaussian(key_list[1], (TOKENS, 2, KR // 2), 1.0, 6.0, ((0, 8), (2, 4))),
        "q_head_grad": bell_draw_with(key_list[2], (TOKENS, HEADS * DN), TOKENS ** -0.5, 0.1875, ((0, 8),), (0, 1, 8, 2.0)),
        "k_head_grad": bell_draw_with(key_list[3], (TOKENS, HEADS * DN), TOKENS ** -0.5, 0.1875, ((0, 8),), (0, 1, 8, 2.0)),
        "q_heads": gaussian(key_list[4], (TOKENS, HEADS * DN), 1.0, 6.0, ((0, 8), (1, 4))),
        "k_heads": gaussian(key_list[5], (TOKENS, HEADS * DN), 1.0, 6.0, ((0, 8), (1, 4))),
        "query_pick": touch_ends(jax.random.randint(key_list[6], (N_DP, PICKS, HEADS), 0, TOK_DEV), jax.random.fold_in(key_list[6], 1), 0, TOK_DEV - 1).astype(jnp.int32),
        "key_pick": touch_ends(jax.random.randint(key_list[7], (N_DP, PICKS, HEADS), 0, TOK_DEV), jax.random.fold_in(key_list[7], 1), 0, TOK_DEV - 1).astype(jnp.int32),
        "q_weight": gaussian(key_list[8], (2 * HEADS, QR // 2, DN), 1.0, 6.0, ((0, 8), (1, 4)), jnp.float32),
        "k_weight": gaussian(key_list[9], (2 * HEADS, KR // 2, DN), 1.0, 6.0, ((0, 8), (1, 4)), jnp.float32),
        "q_moment": gaussian(key_list[10], (2 * HEADS, QR // 2, DN), 1.0, 6.0, ((0, 8), (1, 4)), jnp.float32),
        "k_moment": gaussian(key_list[11], (2 * HEADS, KR // 2, DN), 1.0, 6.0, ((0, 8), (1, 4)), jnp.float32),
    }


MOMENTUM = 0.95
STEP_SIZE = 1.0
DECAY = 0.1
CLIP_LEVEL = 0.1
SCORE_SCALE = 1.0 / math.sqrt(192.0)
COEFF_A = 3.4445
COEFF_B = -4.775
COEFF_C = 2.0315
HIGHEST = lax.Precision.HIGHEST

def grad_slots(latent, head_grad):
    flat = latent.reshape(latent.shape[0], -1)
    total = jnp.dot(flat.T, head_grad, preferred_element_type=jnp.float32)
    rows_all = total.shape[0]
    total = total.reshape(2, rows_all // 2, HEADS, DN).transpose(0, 2, 1, 3)
    return total.reshape(2 * HEADS, rows_all // 2, DN)

def to_heads(slots):
    count, half_rows, width = slots.shape
    stacked = slots.reshape(2, count // 2, half_rows, width).transpose(1, 0, 2, 3)
    return stacked.reshape(count // 2, 2 * half_rows, width)

def to_slots(stacked):
    heads, rows_all, width = stacked.shape
    split = stacked.reshape(heads, 2, rows_all // 2, width).transpose(1, 0, 2, 3)
    return split.reshape(2 * heads, rows_all // 2, width)

def gramians(stacked):
    return jnp.einsum('hrc,hrd->hcd', stacked, stacked, precision=HIGHEST)

def polar(stacked):
    grams = gramians(stacked)
    scale = 1.0 / jnp.sqrt(jnp.trace(grams, axis1=1, axis2=2) + 1.0)
    current = stacked * scale[:, None, None]
    grams = grams * (scale * scale)[:, None, None]
    for step in range(ITERS):
        square = jnp.einsum('hcd,hde->hce', grams, grams, precision=HIGHEST)
        mixer = COEFF_B * grams + COEFF_C * square
        current = COEFF_A * current + jnp.einsum('hrc,hcd->hrd', current, mixer, precision=HIGHEST)
        if step + 1 < ITERS:
            grams = gramians(current)
    return current

def head_peaks(q_heads, k_heads, query_pick, key_pick):
    q_cube = q_heads.reshape(N_DP, TOK_DEV, HEADS, DN)
    k_cube = k_heads.reshape(N_DP, TOK_DEV, HEADS, DN)
    picked_q = jnp.take_along_axis(q_cube, query_pick.astype(jnp.int32)[..., None], axis=1)
    picked_k = jnp.take_along_axis(k_cube, key_pick.astype(jnp.int32)[..., None], axis=1)
    scores = lax.optimization_barrier(jnp.sum(picked_q.astype(jnp.float32) * picked_k.astype(jnp.float32), axis=3)) * SCORE_SCALE
    return lax.optimization_barrier(jnp.max(scores, axis=(0, 1)))

def reference(q_latent, kv_latent, q_head_grad, k_head_grad, q_heads, k_heads, query_pick, key_pick, q_weight, k_weight, q_moment, k_moment):
    q_moment_new = MOMENTUM * q_moment + grad_slots(q_latent, q_head_grad)
    k_moment_new = MOMENTUM * k_moment + grad_slots(kv_latent, k_head_grad)
    q_ortho = to_slots(polar(to_heads(q_moment_new)))
    k_ortho = to_slots(polar(to_heads(k_moment_new)))
    peak = head_peaks(q_heads, k_heads, query_pick, key_pick)
    shrink = jnp.sqrt(CLIP_LEVEL / jnp.maximum(peak, CLIP_LEVEL))
    shrink_slots = jnp.concatenate([shrink, shrink])[:, None, None]
    keep = 1.0 - STEP_SIZE * DECAY
    q_weight_new = (q_weight * keep - STEP_SIZE * 0.2 * math.sqrt(QR) * q_ortho) * shrink_slots
    k_weight_new = (k_weight * keep - STEP_SIZE * 0.2 * math.sqrt(KR) * k_ortho) * shrink_slots
    return (q_weight_new, k_weight_new, q_moment_new, k_moment_new)
```

```python
import functools
import math

import jax
import jax.numpy as jnp
from jax import lax
from jax.experimental import pallas as pl
from jax.experimental.pallas import tpu as pltpu
from jax.sharding import PartitionSpec as P

ITERS = 5
MOMENTUM = 0.95
STEP_SIZE = 1.0
DECAY = 0.1
CLIP_LEVEL = 0.1
SCORE_SCALE = 1.0 / math.sqrt(192.0)
COEFF_A = 3.4445
COEFF_B = -4.775
COEFF_C = 2.0315
HIGHEST = lax.Precision.HIGHEST
SUB = 8
LANES = 128
LOW = -1e30
FIRST_SHARE = 0.66


VMEM = pl.BlockSpec(memory_space=pltpu.VMEM)


def f32(*shape):
    return jax.ShapeDtypeStruct(shape, jnp.float32)


def call(body, outs, *args, scratch=(), name):
    return pl.pallas_call(
        body,
        out_shape=outs,
        in_specs=[VMEM] * len(args),
        out_specs=[VMEM] * len(outs),
        scratch_shapes=scratch,
        name=name,
    )(*args)


def product(x, y, dims):
    return lax.dot_general(
        x, y, (dims, ((), ())), precision=HIGHEST, preferred_element_type=jnp.float32
    )


def peak_rows(q_heads, k_heads, query_pick, key_pick, first_head):
    tokens = q_heads.shape[0]
    heads, picks = query_pick.shape
    width = q_heads.shape[1] // heads
    spot = lax.broadcasted_iota(jnp.int32, (SUB, LANES), 1)
    token = lax.broadcasted_iota(jnp.int32, (tokens, picks), 0)
    rows = jnp.full((SUB, LANES), LOW, jnp.float32)
    for head in range(heads):
        picked = []
        for pick, held in ((query_pick, q_heads), (key_pick, k_heads)):
            chosen = (token == pick[head : head + 1, :]).astype(jnp.float32).astype(jnp.bfloat16)
            values = held[:, head * width : (head + 1) * width]
            picked.append(
                lax.dot_general(
                    chosen, values, (((0,), (0,)), ((), ())), preferred_element_type=jnp.float32
                )
            )
        scores = jnp.sum(picked[0] * picked[1], axis=1, keepdims=True) * SCORE_SCALE
        top = jnp.max(scores, axis=0, keepdims=True)
        rows = jnp.where(spot == first_head + head, top, rows)
    return rows


def terms_body(
    ql, kl, qg, kg, qh, kh, qp, kp, xs, ka, *rest, head_count, q_rows, k_rows, share, width
):
    *zb, tiles = rest
    device = lax.axis_index("dp")
    for half in range(2):
        for latent, grad, rows, start in ((ql, qg, q_rows, 0), (kl, kg, k_rows, q_rows)):
            term = jnp.dot(
                latent[half * rows : (half + 1) * rows, :],
                grad[...],
                preferred_element_type=jnp.float32,
            )
            for head in range(head_count):
                tiles[half * head_count + head, start : start + rows, :] = term[
                    :, head * width : (head + 1) * width
                ]
    row_count = q_rows + k_rows
    late = row_count - share
    for step in range(2 * head_count):
        tile = tiles[device ^ step]
        outer, inner = step // 2, step % 2
        (xs if inner else ka)[outer * share : (outer + 1) * share, :] = tile[:share]
        zb[outer][inner * late : (inner + 1) * late, :] = tile[share:]
    local_heads = qp.shape[0]
    rows = peak_rows(qh, kh, qp, kp, lax.axis_index("mp") * local_heads)
    xs[head_count * share :, :] = rows
    ka[head_count * share :, :] = rows


def inner_sum_body(ka, rx, *outs):
    count = len(outs)
    share = (ka.shape[0] - SUB) // count
    rows = jnp.maximum(ka[count * share :, :], rx[count * share :, :])
    for step, out in enumerate(outs):
        part = slice(step * share, (step + 1) * share)
        out[:share, :] = ka[part, :] + rx[part, :]
        out[share:, :] = rows


def outer_sum_body(*refs):
    *parts, keep, send = refs
    late = keep.shape[0]
    total = parts[0][...]
    for part in parts[1:]:
        total = total + part[...]
    keep[...] = total[:late]
    send[...] = total[late:]


def sum_over_dp(ql, kl, qg, kg, qh, kh, qp, kp, q_rows, k_rows, width):
    count = lax.axis_size("dp")
    head_count = count // 2
    row_count = q_rows + k_rows
    share = int(row_count * FIRST_SHARE) // SUB * SUB
    late = row_count - share
    body = functools.partial(
        terms_body,
        head_count=head_count,
        q_rows=q_rows,
        k_rows=k_rows,
        share=share,
        width=width,
    )
    first = f32(head_count * share + SUB, width)
    xs, ka, *zb = call(
        body,
        [first, first] + [f32(2 * late, width)] * head_count,
        ql, kl, qg, kg, qh, kh, qp, kp,
        scratch=[pltpu.VMEM((count, row_count, width), jnp.float32)],
        name="terms",
    )
    across = [(source, source ^ 1) for source in range(count)]
    steps = list(range(2, head_count)) + [1]

    def along(value, step):
        return lax.ppermute(value, "dp", [(source, source ^ (2 * step)) for source in range(count)])

    rx = lax.ppermute(xs, "dp", across)
    rz = [along(zb[step], step) for step in steps]
    sums = call(inner_sum_body, [f32(share + SUB, width)] * head_count, ka, rx, name="inner_sum")
    late_keep, late_send = call(
        outer_sum_body, [f32(late, width)] * 2, zb[0], *rz, name="outer_sum"
    )
    late_other = lax.ppermute(late_send, "dp", across)
    others = [along(sums[step], step) for step in steps]
    return [sums[0], *others], [late_keep, late_other]


def scatter_over_dp(ql, kl, qg, kg, qh, kh, qp, kp, q_rows, k_rows, width):
    count = lax.axis_size("dp")
    head_count = count // 2
    terms = []
    for latent, grad, rows in ((ql, qg, q_rows), (kl, kg, k_rows)):
        term = jnp.dot(latent, grad, preferred_element_type=jnp.float32)
        term = term.reshape(2, rows, head_count, width).transpose(0, 2, 1, 3)
        terms.append(term.reshape(count, rows, width))
    own = lax.psum_scatter(
        jnp.concatenate(terms, axis=1), "dp", scatter_dimension=0, tiled=True
    )[0]

    def body(qh, kh, qp, kp, rows):
        rows[...] = peak_rows(qh, kh, qp, kp, lax.axis_index("mp") * qp.shape[0])

    (rows,) = call(body, [f32(SUB, width)], qh, kh, qp, kp, name="scores")
    rows = lax.pmax(rows, "dp")
    late = SUB
    return [jnp.concatenate([own[:-late], rows], axis=0)], [own[-late:]]


def gram_body(*refs, early, q_rows):
    mq, mk = refs[0], refs[1]
    parts = refs[2:-4]
    mq_new, mk_new, keep, send = refs[-4:]
    first, second = parts[:early], parts[early:]
    share = first[0].shape[0] - SUB
    total = first[0][:share, :]
    rows = first[0][share:, :]
    for part in first[1:]:
        total = total + part[:share, :]
        rows = jnp.maximum(rows, part[share:, :])
    late = second[0][...]
    for part in second[1:]:
        late = late + part[...]
    own = jnp.concatenate([total, late], axis=0)
    q = MOMENTUM * mq[...] + own[:q_rows]
    k = MOMENTUM * mk[...] + own[q_rows:]
    mq_new[...] = q
    mk_new[...] = k
    q_gram = product(q, q, ((0,), (0,)))
    k_gram = product(k, k, ((0,), (0,)))
    odd = lax.axis_index("mp") % 2 == 1
    width = q_gram.shape[0]
    keep[:width, :] = jnp.where(odd, k_gram, q_gram)
    send[:width, :] = jnp.where(odd, q_gram, k_gram)
    keep[width:, :] = rows
    send[width:, :] = rows


def join_body(keep, other, out):
    width = keep.shape[0] - SUB
    out[:width, :] = keep[:width, :] + other[:width, :]
    out[width:, :] = jnp.maximum(keep[width:, :], other[width:, :])


def polar_body(*refs, head_count):
    *parts, mixer_out, shrink_out = refs
    width = parts[0].shape[0] - SUB
    gram = parts[0][:width, :]
    rows = parts[0][width:, :]
    for part in parts[1:]:
        gram = gram + part[:width, :]
        rows = jnp.maximum(rows, part[width:, :])
    spot = lax.broadcasted_iota(jnp.int32, rows.shape, 1)
    own = lax.axis_index("dp") % head_count
    peak = jnp.max(jnp.where(spot == own, rows, LOW), axis=(0, 1), keepdims=True)
    shrink = jnp.sqrt(CLIP_LEVEL / jnp.maximum(peak, CLIP_LEVEL))
    shrink_out[...] = jnp.broadcast_to(shrink, shrink_out.shape)
    line = lax.broadcasted_iota(jnp.int32, gram.shape, 0)
    diagonal = line == lax.broadcasted_iota(jnp.int32, gram.shape, 1)
    trace = jnp.sum(jnp.where(diagonal, gram, 0.0), axis=(0, 1), keepdims=True)
    scale = 1.0 / jnp.sqrt(trace + 1.0)
    gram = gram * (scale * scale)
    unit = jnp.where(diagonal, COEFF_A, 0.0)
    mix = None
    plain = ((1,), (0,))
    for step in range(ITERS):
        square = product(gram, gram, plain)
        mixer = unit + (COEFF_B * gram + COEFF_C * square)
        mix = mixer * scale if mix is None else product(mix, mixer, plain)
        if step + 1 < ITERS:
            gram = product(mixer, product(gram, mixer, plain), plain)
    mixer_out[...] = mix


def apply_body(mq, mk, wq, wk, mine, other, shrink, wq_new, wk_new, *, q_norm, k_norm):
    odd = lax.axis_index("mp") % 2 == 1
    q_mix = jnp.where(odd, other[...], mine[...])
    k_mix = jnp.where(odd, mine[...], other[...])
    keep = 1.0 - STEP_SIZE * DECAY
    plain = ((1,), (0,))
    factor = shrink[0:1, :]
    wq_new[...] = (wq[...] * keep - q_norm * product(mq[...], q_mix, plain)) * factor
    wk_new[...] = (wk[...] * keep - k_norm * product(mk[...], k_mix, plain)) * factor


def local(
    q_latent,
    kv_latent,
    q_head_grad,
    k_head_grad,
    q_heads,
    k_heads,
    query_pick,
    key_pick,
    q_weight,
    k_weight,
    q_moment,
    k_moment,
):
    dp, mp = lax.axis_size("dp"), lax.axis_size("mp")
    head_count = dp // 2
    tokens = q_latent.shape[0]
    q_rows, k_rows = q_latent.shape[2], kv_latent.shape[2]
    width = q_moment.shape[2]
    ql = jnp.transpose(q_latent, (1, 2, 0)).reshape(2 * q_rows, tokens)
    kl = jnp.transpose(kv_latent, (1, 2, 0)).reshape(2 * k_rows, tokens)
    qp = jnp.transpose(query_pick[0], (1, 0))
    kp = jnp.transpose(key_pick[0], (1, 0))
    direct = dp <= 16 and dp & (dp - 1) == 0
    reduce = sum_over_dp if direct else scatter_over_dp
    first, second = reduce(
        ql, kl, q_head_grad, k_head_grad, q_heads, k_heads, qp, kp, q_rows, k_rows, width
    )
    mq_new, mk_new, keep, send = call(
        functools.partial(gram_body, early=len(first), q_rows=q_rows),
        [f32(q_rows, width), f32(k_rows, width)] + [f32(width + SUB, width)] * 2,
        q_moment[0], k_moment[0], *first, *second,
        name="gram",
    )
    pair = [(source, source ^ 1) for source in range(mp)]
    other = lax.ppermute(send, "mp", pair)
    (joined,) = call(join_body, [f32(width + SUB, width)], keep, other, name="join")
    parts = [joined]
    for far in (1, 0):
        for near in range(mp // 2):
            if far or near:
                route = [
                    (d * mp + m, (d + far * head_count) % dp * mp + (m + 2 * near) % mp)
                    for d in range(dp)
                    for m in range(mp)
                ]
                parts.append(lax.ppermute(joined, ("dp", "mp"), route))
    mine, shrink = call(
        functools.partial(polar_body, head_count=head_count),
        [f32(width, width), f32(SUB, width)],
        *parts,
        name="polar",
    )
    theirs = lax.ppermute(mine, "mp", pair)
    wq_new, wk_new = call(
        functools.partial(
            apply_body,
            q_norm=STEP_SIZE * 0.2 * math.sqrt(2 * q_rows * mp),
            k_norm=STEP_SIZE * 0.2 * math.sqrt(2 * k_rows * mp),
        ),
        [f32(q_rows, width), f32(k_rows, width)],
        mq_new, mk_new, q_weight[0], k_weight[0], mine, theirs, shrink,
        name="apply",
    )
    return (wq_new[None], wk_new[None], mq_new[None], mk_new[None])


def solution(mesh):
    in_specs = (
        P("dp", None, "mp"),
        P("dp", None, "mp"),
        P("dp", None),
        P("dp", None),
        P("dp", "mp"),
        P("dp", "mp"),
        P("dp", None, "mp"),
        P("dp", None, "mp"),
        P("dp", "mp", None),
        P("dp", "mp", None),
        P("dp", "mp", None),
        P("dp", "mp", None),
    )
    out_specs = (P("dp", "mp", None), P("dp", "mp", None), P("dp", "mp", None), P("dp", "mp", None))
    return jax.shard_map(local, mesh=mesh, in_specs=in_specs, out_specs=out_specs, check_vma=False)
```

```python
import functools
import math

import jax
import jax.numpy as jnp
from jax import lax
from jax.experimental import pallas as pl
from jax.experimental.pallas import tpu as pltpu
from jax.sharding import PartitionSpec as P

ITERS = 5
MOMENTUM = 0.95
STEP_SIZE = 1.0
DECAY = 0.1
CLIP_LEVEL = 0.1
SCORE_SCALE = 1.0 / math.sqrt(192.0)
COEFF_A = 3.4445
COEFF_B = -4.775
COEFF_C = 2.0315
HIGHEST = lax.Precision.HIGHEST
SUB = 8
LANES = 128
LOW = -1e30
FIRST_SHARE = 0.66


VMEM = pl.BlockSpec(memory_space=pltpu.VMEM)
ANY = pl.BlockSpec(memory_space=pl.ANY)


def f32(*shape):
    return jax.ShapeDtypeStruct(shape, jnp.float32)


def call(body, outs, *args, scratch=(), name, limit=4, fetched=False):
    if fetched:
        args = [pltpu.with_memory_space_constraint(arg, pltpu.HBM) for arg in args]
    return pl.pallas_call(
        body,
        out_shape=outs,
        in_specs=[ANY if fetched else VMEM] * len(args),
        out_specs=[VMEM] * len(outs),
        scratch_shapes=scratch,
        compiler_params=pltpu.CompilerParams(vmem_limit_bytes=limit * 2**20),
        name=name,
    )(*args)


def product(x, y, dims):
    return lax.dot_general(
        x, y, (dims, ((), ())), precision=HIGHEST, preferred_element_type=jnp.float32
    )


def peak_rows(q_heads, k_heads, query_pick, key_pick, first_head):
    tokens = q_heads.shape[0]
    heads, picks = query_pick.shape
    width = q_heads.shape[1] // heads
    spot = lax.broadcasted_iota(jnp.int32, (SUB, LANES), 1)
    token = lax.broadcasted_iota(jnp.int32, (tokens, picks), 0)
    rows = jnp.full((SUB, LANES), LOW, jnp.float32)
    for head in range(heads):
        picked = []
        for pick, held in ((query_pick, q_heads), (key_pick, k_heads)):
            chosen = (token == pick[head : head + 1, :]).astype(jnp.float32).astype(jnp.bfloat16)
            values = held[:, head * width : (head + 1) * width]
            picked.append(
                lax.dot_general(
                    chosen, values, (((0,), (0,)), ((), ())), preferred_element_type=jnp.float32
                )
            )
        scores = jnp.sum(picked[0] * picked[1], axis=1, keepdims=True) * SCORE_SCALE
        top = jnp.max(scores, axis=0, keepdims=True)
        rows = jnp.where(spot == first_head + head, top, rows)
    return rows


def terms_body(*refs, head_count, q_rows, k_rows, share, width):
    sources, (xs, ka, *zb), held = refs[:8], refs[8 : 10 + head_count], refs[10 + head_count :]
    ql, kl, qg, kg, qh, kh, qp, kp, tiles, sems = held
    copies = [
        pltpu.make_async_copy(source, kept, sems.at[n])
        for n, (source, kept) in enumerate(zip(sources, held[:8]))
    ]
    for n in (0, 2, 1, 3, 4, 5, 6, 7):
        copies[n].start()
    device = lax.axis_index("dp")
    for latent, grad, rows, start, n in ((ql, qg, q_rows, 0, 0), (kl, kg, k_rows, q_rows, 1)):
        copies[n].wait()
        copies[n + 2].wait()
        for half in range(2):
            term = jnp.dot(
                latent[half * rows : (half + 1) * rows, :],
                grad[...],
                preferred_element_type=jnp.float32,
            )
            for head in range(head_count):
                tiles[half * head_count + head, start : start + rows, :] = term[
                    :, head * width : (head + 1) * width
                ]
    row_count = q_rows + k_rows
    late = row_count - share
    for step in range(2 * head_count):
        tile = tiles[device ^ step]
        outer, inner = step // 2, step % 2
        (xs if inner else ka)[outer * share : (outer + 1) * share, :] = tile[:share]
        zb[outer][inner * late : (inner + 1) * late, :] = tile[share:]
    for copy in copies[4:]:
        copy.wait()
    rows = peak_rows(qh, kh, qp, kp, lax.axis_index("mp") * qp.shape[0])
    xs[head_count * share :, :] = rows
    ka[head_count * share :, :] = rows


def inner_sum_body(ka, rx, *outs):
    count = len(outs)
    share = (ka.shape[0] - SUB) // count
    rows = jnp.maximum(ka[count * share :, :], rx[count * share :, :])
    for step, out in enumerate(outs):
        part = slice(step * share, (step + 1) * share)
        out[:share, :] = ka[part, :] + rx[part, :]
        out[share:, :] = rows


def outer_sum_body(*refs):
    *parts, keep, send = refs
    late = keep.shape[0]
    total = parts[0][...]
    for part in parts[1:]:
        total = total + part[...]
    keep[...] = total[:late]
    send[...] = total[late:]


def sum_over_dp(ql, kl, qg, kg, qh, kh, qp, kp, q_rows, k_rows, width):
    count = lax.axis_size("dp")
    head_count = count // 2
    row_count = q_rows + k_rows
    share = int(row_count * FIRST_SHARE) // SUB * SUB
    late = row_count - share
    body = functools.partial(
        terms_body,
        head_count=head_count,
        q_rows=q_rows,
        k_rows=k_rows,
        share=share,
        width=width,
    )
    first = f32(head_count * share + SUB, width)
    args = (ql, kl, qg, kg, qh, kh, qp, kp)
    xs, ka, *zb = call(
        body,
        [first, first] + [f32(2 * late, width)] * head_count,
        *args,
        scratch=[pltpu.VMEM(arg.shape, arg.dtype) for arg in args]
        + [pltpu.VMEM((count, row_count, width), jnp.float32), pltpu.SemaphoreType.DMA((8,))],
        name="terms",
        limit=12,
        fetched=True,
    )
    across = [(source, source ^ 1) for source in range(count)]
    steps = list(range(2, head_count)) + [1]

    def along(value, step):
        return lax.ppermute(value, "dp", [(source, source ^ (2 * step)) for source in range(count)])

    rx = lax.ppermute(xs, "dp", across)
    rz = [along(zb[step], step) for step in steps]
    sums = call(inner_sum_body, [f32(share + SUB, width)] * head_count, ka, rx, name="inner_sum")
    late_keep, late_send = call(
        outer_sum_body, [f32(late, width)] * 2, zb[0], *rz, name="outer_sum"
    )
    late_other = lax.ppermute(late_send, "dp", across)
    others = [along(sums[step], step) for step in steps]
    return [sums[0], *others], [late_keep, late_other]


def scatter_over_dp(ql, kl, qg, kg, qh, kh, qp, kp, q_rows, k_rows, width):
    count = lax.axis_size("dp")
    head_count = count // 2
    terms = []
    for latent, grad, rows in ((ql, qg, q_rows), (kl, kg, k_rows)):
        term = jnp.dot(latent, grad, preferred_element_type=jnp.float32)
        term = term.reshape(2, rows, head_count, width).transpose(0, 2, 1, 3)
        terms.append(term.reshape(count, rows, width))
    own = lax.psum_scatter(
        jnp.concatenate(terms, axis=1), "dp", scatter_dimension=0, tiled=True
    )[0]

    def body(qh, kh, qp, kp, rows):
        rows[...] = peak_rows(qh, kh, qp, kp, lax.axis_index("mp") * qp.shape[0])

    (rows,) = call(body, [f32(SUB, width)], qh, kh, qp, kp, name="scores")
    rows = lax.pmax(rows, "dp")
    late = SUB
    return [jnp.concatenate([own[:-late], rows], axis=0)], [own[-late:]]


def folded(gram, rows):
    width = gram.shape[0]
    half = width // 2
    line = lax.broadcasted_iota(jnp.int32, (half, width), 0)
    lane = lax.broadcasted_iota(jnp.int32, (half, width), 1)
    low = pltpu.roll(gram[half:, :], half, 1)
    diagonal = jnp.sum(jnp.where(line == lane, low, 0.0), axis=0, keepdims=True)
    spare = lax.broadcasted_iota(jnp.int32, rows.shape, 0)
    return jnp.where((lane < half) & (line > lane), low, gram[:half, :]), jnp.where(
        spare == 0, diagonal, rows
    )


def unfolded(top, rows):
    half, width = top.shape
    line = lax.broadcasted_iota(jnp.int32, (half, width), 0)
    lane = lax.broadcasted_iota(jnp.int32, (half, width), 1)
    turned = jnp.transpose(jnp.concatenate([top, jnp.zeros_like(top)], axis=0))
    over = turned[:half, :]
    low = jnp.where(line > lane, top, jnp.where(line == lane, rows[0:1, :], over))
    above = jnp.where((lane < half) & (line > lane), over, top)
    below = jnp.where(lane < half, turned[half:, :], pltpu.roll(low, half, 1))
    return jnp.concatenate([above, below], axis=0)


def gathered(parts):
    half = parts[0].shape[0] - SUB
    top, rows, high = parts[0][:half, :], parts[0][half:, :], parts[0][half:, :]
    for part in parts[1:]:
        top = top + part[:half, :]
        rows = rows + part[half:, :]
        high = jnp.maximum(high, part[half:, :])
    spare = lax.broadcasted_iota(jnp.int32, rows.shape, 0)
    return top, jnp.where(spare == 0, rows, high)


def gram_body(*refs, early, q_rows):
    mq, mk = refs[0], refs[1]
    parts = refs[2:-4]
    mq_new, mk_new, keep, send = refs[-4:]
    first, second = parts[:early], parts[early:]
    share = first[0].shape[0] - SUB
    total = first[0][:share, :]
    rows = first[0][share:, :]
    for part in first[1:]:
        total = total + part[:share, :]
        rows = jnp.maximum(rows, part[share:, :])
    late = second[0][...]
    for part in second[1:]:
        late = late + part[...]
    own = jnp.concatenate([total, late], axis=0)
    q = MOMENTUM * mq[...] + own[:q_rows]
    k = MOMENTUM * mk[...] + own[q_rows:]
    mq_new[...] = q
    mk_new[...] = k
    q_gram = product(q, q, ((0,), (0,)))
    k_gram = product(k, k, ((0,), (0,)))
    odd = lax.axis_index("mp") % 2 == 1
    half = q_gram.shape[0] // 2
    q_fold, q_rest = folded(q_gram, rows)
    k_fold, k_rest = folded(k_gram, rows)
    keep[:half, :] = jnp.where(odd, k_fold, q_fold)
    send[:half, :] = jnp.where(odd, q_fold, k_fold)
    keep[half:, :] = jnp.where(odd, k_rest, q_rest)
    send[half:, :] = jnp.where(odd, q_rest, k_rest)


def join_body(keep, other, out):
    half = keep.shape[0] - SUB
    out[:half, :], out[half:, :] = gathered((keep, other))


def polar_body(*refs, head_count):
    *parts, mixer_out, shrink_out = refs
    top, rows = gathered(parts)
    gram = unfolded(top, rows)
    rows = rows[1:, :]
    spot = lax.broadcasted_iota(jnp.int32, rows.shape, 1)
    own = lax.axis_index("dp") % head_count
    peak = jnp.max(jnp.where(spot == own, rows, LOW), axis=(0, 1), keepdims=True)
    shrink = jnp.sqrt(CLIP_LEVEL / jnp.maximum(peak, CLIP_LEVEL))
    shrink_out[...] = jnp.broadcast_to(shrink, shrink_out.shape)
    line = lax.broadcasted_iota(jnp.int32, gram.shape, 0)
    diagonal = line == lax.broadcasted_iota(jnp.int32, gram.shape, 1)
    trace = jnp.sum(jnp.where(diagonal, gram, 0.0), axis=(0, 1), keepdims=True)
    scale = 1.0 / jnp.sqrt(trace + 1.0)
    gram = gram * (scale * scale)
    unit = jnp.where(diagonal, COEFF_A, 0.0)
    mix = None
    plain = ((1,), (0,))
    for step in range(ITERS):
        square = product(gram, gram, plain)
        mixer = unit + (COEFF_B * gram + COEFF_C * square)
        mix = mixer * scale if mix is None else product(mix, mixer, plain)
        if step + 1 < ITERS:
            gram = product(mixer, product(gram, mixer, plain), plain)
    mixer_out[...] = mix


def apply_body(mq, mk, wq, wk, mine, other, shrink, wq_new, wk_new, *, q_norm, k_norm):
    odd = lax.axis_index("mp") % 2 == 1
    q_mix = jnp.where(odd, other[...], mine[...])
    k_mix = jnp.where(odd, mine[...], other[...])
    keep = 1.0 - STEP_SIZE * DECAY
    plain = ((1,), (0,))
    factor = shrink[0:1, :]
    wq_new[...] = (wq[...] * keep - q_norm * product(mq[...], q_mix, plain)) * factor
    wk_new[...] = (wk[...] * keep - k_norm * product(mk[...], k_mix, plain)) * factor


def local(
    q_latent,
    kv_latent,
    q_head_grad,
    k_head_grad,
    q_heads,
    k_heads,
    query_pick,
    key_pick,
    q_weight,
    k_weight,
    q_moment,
    k_moment,
):
    dp, mp = lax.axis_size("dp"), lax.axis_size("mp")
    head_count = dp // 2
    tokens = q_latent.shape[0]
    q_rows, k_rows = q_latent.shape[2], kv_latent.shape[2]
    width = q_moment.shape[2]
    ql = jnp.transpose(q_latent, (1, 2, 0)).reshape(2 * q_rows, tokens)
    kl = jnp.transpose(kv_latent, (1, 2, 0)).reshape(2 * k_rows, tokens)
    qp = jnp.transpose(query_pick[0], (1, 0))
    kp = jnp.transpose(key_pick[0], (1, 0))
    direct = dp <= 16 and dp & (dp - 1) == 0
    reduce = sum_over_dp if direct else scatter_over_dp
    first, second = reduce(
        ql, kl, q_head_grad, k_head_grad, q_heads, k_heads, qp, kp, q_rows, k_rows, width
    )
    mq_new, mk_new, keep, send = call(
        functools.partial(gram_body, early=len(first), q_rows=q_rows),
        [f32(q_rows, width), f32(k_rows, width)] + [f32(width // 2 + SUB, width)] * 2,
        q_moment[0], k_moment[0], *first, *second,
        name="gram",
    )
    pair = [(source, source ^ 1) for source in range(mp)]
    other = lax.ppermute(send, "mp", pair)
    (joined,) = call(join_body, [f32(width // 2 + SUB, width)], keep, other, name="join")
    parts = [joined]
    for far in (1, 0):
        for near in range(mp // 2):
            if far or near:
                route = [
                    (d * mp + m, (d + far * head_count) % dp * mp + (m + 2 * near) % mp)
                    for d in range(dp)
                    for m in range(mp)
                ]
                parts.append(lax.ppermute(joined, ("dp", "mp"), route))
    mine, shrink = call(
        functools.partial(polar_body, head_count=head_count),
        [f32(width, width), f32(SUB, width)],
        *parts,
        name="polar",
    )
    theirs = lax.ppermute(mine, "mp", pair)
    wq_new, wk_new = call(
        functools.partial(
            apply_body,
            q_norm=STEP_SIZE * 0.2 * math.sqrt(2 * q_rows * mp),
            k_norm=STEP_SIZE * 0.2 * math.sqrt(2 * k_rows * mp),
        ),
        [f32(q_rows, width), f32(k_rows, width)],
        mq_new, mk_new, q_weight[0], k_weight[0], mine, theirs, shrink,
        name="apply",
    )
    return (wq_new[None], wk_new[None], mq_new[None], mk_new[None])


def solution(mesh):
    in_specs = (
        P("dp", None, "mp"),
        P("dp", None, "mp"),
        P("dp", None),
        P("dp", None),
        P("dp", "mp"),
        P("dp", "mp"),
        P("dp", None, "mp"),
        P("dp", None, "mp"),
        P("dp", "mp", None),
        P("dp", "mp", None),
        P("dp", "mp", None),
        P("dp", "mp", None),
    )
    out_specs = (P("dp", "mp", None), P("dp", "mp", None), P("dp", "mp", None), P("dp", "mp", None))
    return jax.shard_map(local, mesh=mesh, in_specs=in_specs, out_specs=out_specs, check_vma=False)
```

```python
import functools
import math

import jax
import jax.numpy as jnp
from jax import lax
from jax.experimental import pallas as pl
from jax.experimental.pallas import tpu as pltpu
from jax.sharding import PartitionSpec as P


ITERS = 5
MOMENTUM = 0.95
STEP_SIZE = 1.0
DECAY = 0.1
CLIP_LEVEL = 0.1
SCORE_SCALE = 1.0 / math.sqrt(192.0)
COEFF_A = 3.4445
COEFF_B = -4.775
COEFF_C = 2.0315
HIGHEST = lax.Precision.HIGHEST
SUB = 8
LANES = 128
LOW = -1e30
FIRST_SHARES = (0.66,)


VMEM = pl.BlockSpec(memory_space=pltpu.VMEM)
ANY = pl.BlockSpec(memory_space=pl.ANY)


def f32(*shape):
    return jax.ShapeDtypeStruct(shape, jnp.float32)


def call(body, outs, *args, scratch=(), limit=4, fetched=False):
    if fetched:
        args = [pltpu.with_memory_space_constraint(arg, pltpu.HBM) for arg in args]
    return pl.pallas_call(
        body,
        out_shape=outs,
        in_specs=[ANY if fetched else VMEM] * len(args),
        out_specs=[VMEM if isinstance(out, jax.ShapeDtypeStruct) else ANY for out in outs],
        scratch_shapes=scratch,
        compiler_params=pltpu.CompilerParams(vmem_limit_bytes=limit * 2**20),
    )(*args)


def product(x, y, dims):
    return lax.dot_general(
        x, y, (dims, ((), ())), precision=HIGHEST, preferred_element_type=jnp.float32
    )


def pieces(x):
    high = x.astype(jnp.bfloat16)
    rest = x - high.astype(jnp.float32)
    middle = rest.astype(jnp.bfloat16)
    return high, middle, (rest - middle.astype(jnp.float32)).astype(jnp.bfloat16)


def left(x):
    high, middle, low = x
    return jnp.concatenate([high, middle], axis=1), jnp.concatenate([high, low], axis=1)


def right(x):
    high, middle, low = x
    pair = jnp.concatenate([high, middle], axis=1)
    return jnp.concatenate([pair, pair], axis=0), jnp.concatenate([low, high], axis=0)


def stacked(x, y):
    four = jnp.dot(x[0], y[0], preferred_element_type=jnp.float32)
    two = jnp.dot(x[1], y[1], preferred_element_type=jnp.float32)
    width = two.shape[1]
    return four[:, :width] + (four[:, width:] + two)


def peak_rows(q_heads, k_heads, query_pick, key_pick, first_head):
    tokens = q_heads.shape[0]
    heads, picks = query_pick.shape
    width = q_heads.shape[1] // heads
    spot = lax.broadcasted_iota(jnp.int32, (SUB, LANES), 1)
    token = lax.broadcasted_iota(jnp.int32, (tokens, picks), 0)
    rows = jnp.full((SUB, LANES), LOW, jnp.float32)
    for head in range(heads):
        picked = []
        for pick, held in ((query_pick, q_heads), (key_pick, k_heads)):
            chosen = (token == pick[head : head + 1, :]).astype(jnp.float32).astype(jnp.bfloat16)
            values = held[:, head * width : (head + 1) * width]
            picked.append(
                lax.dot_general(
                    chosen, values, (((0,), (0,)), ((), ())), preferred_element_type=jnp.float32
                )
            )
        scores = jnp.sum(picked[0] * picked[1], axis=1, keepdims=True) * SCORE_SCALE
        top = jnp.max(scores, axis=0, keepdims=True)
        rows = jnp.where(spot == first_head + head, top, rows)
    return rows


def terms_body(*refs, head_count, q_rows, k_rows, shares, width):
    sources, held = refs[:8], refs[-10:]
    xs = refs[8 : 8 + len(shares)]
    ka = refs[8 + len(shares) : 8 + 2 * len(shares)]
    zb = refs[8 + 2 * len(shares) : -10]
    ql, kl, qg, kg, qh, kh, qp, kp, tiles, sems = held
    copies = [
        pltpu.make_async_copy(source, kept, sems.at[n])
        for n, (source, kept) in enumerate(zip(sources, held[:8]))
    ]
    for n in (0, 2, 1, 3, 4, 5, 6, 7):
        copies[n].start()
    device = lax.axis_index("dp")
    for latent, grad, rows, start, n in ((ql, qg, q_rows, 0, 0), (kl, kg, k_rows, q_rows, 1)):
        copies[n].wait()
        copies[n + 2].wait()
        for half in range(2):
            term = jnp.dot(
                latent[half * rows : (half + 1) * rows, :],
                grad[...],
                preferred_element_type=jnp.float32,
            )
            for head in range(head_count):
                tiles[half * head_count + head, start : start + rows, :] = term[
                    :, head * width : (head + 1) * width
                ]
    row_count = q_rows + k_rows
    late = row_count - sum(shares)
    for step in range(2 * head_count):
        tile = tiles[device ^ step]
        outer, inner = step // 2, step % 2
        start = 0
        for out, share in zip(xs if inner else ka, shares):
            out[outer * share : (outer + 1) * share, :] = tile[start : start + share]
            start += share
        zb[outer][inner * late : (inner + 1) * late, :] = tile[start:]
    for copy in copies[4:]:
        copy.wait()
    rows = peak_rows(qh, kh, qp, kp, lax.axis_index("mp") * qp.shape[0])
    xs[0][head_count * shares[0] :, :] = rows
    ka[0][head_count * shares[0] :, :] = rows


def inner_sum_body(ka, rx, *outs):
    count = len(outs)
    share = ka.shape[0] // count // SUB * SUB
    for step, out in enumerate(outs):
        part = slice(step * share, (step + 1) * share)
        out[:share, :] = ka[part, :] + rx[part, :]
        if out.shape[0] > share:
            out[share:, :] = jnp.maximum(ka[count * share :, :], rx[count * share :, :])


def outer_sum_body(*refs):
    *parts, keep, send = refs
    late = keep.shape[0]
    total = parts[0][...]
    for part in parts[1:]:
        total = total + part[...]
    keep[...] = total[:late]
    send[...] = total[late:]


def sum_over_dp(ql, kl, qg, kg, qh, kh, qp, kp, q_rows, k_rows, width):
    count = lax.axis_size("dp")
    head_count = count // 2
    row_count = q_rows + k_rows
    shares = [int(row_count * share) // SUB * SUB for share in FIRST_SHARES]
    extra = [SUB] + [0] * (len(shares) - 1)
    late = row_count - sum(shares)
    body = functools.partial(
        terms_body,
        head_count=head_count,
        q_rows=q_rows,
        k_rows=k_rows,
        shares=shares,
        width=width,
    )
    firsts = [f32(head_count * share + more, width) for share, more in zip(shares, extra)]
    args = (ql, kl, qg, kg, qh, kh, qp, kp)
    made = call(
        body,
        firsts + firsts + [f32(2 * late, width)] * head_count,
        *args,
        scratch=[pltpu.VMEM(arg.shape, arg.dtype) for arg in args]
        + [pltpu.VMEM((count, row_count, width), jnp.float32), pltpu.SemaphoreType.DMA((8,))],
        limit=12,
        fetched=True,
    )
    xs, ka, zb = made[: len(shares)], made[len(shares) : 2 * len(shares)], made[2 * len(shares) :]
    across = [(source, source ^ 1) for source in range(count)]
    steps = list(range(2, head_count)) + [1]

    def along(value, step):
        route = [(source, source ^ (2 * step)) for source in range(count)]
        return lax.ppermute(value, "dp", route)

    rx = [lax.ppermute(value, "dp", across) for value in xs]
    rz = [along(zb[step], step) for step in steps]
    firsts = []
    for n, (share, more) in enumerate(zip(shares, extra)):
        rides = [more if step <= (head_count - 1) // 2 else 0 for step in range(head_count)]
        sums = call(
            inner_sum_body,
            [f32(share + ride, width) for ride in rides],
            ka[n], rx[n],
        )
        firsts.append([sums[0]] + [along(sums[step], step) for step in steps])
    late_keep, late_send = call(outer_sum_body, [f32(late, width)] * 2, zb[0], *rz)
    late_other = lax.ppermute(late_send, "dp", across)
    return [*firsts, [late_keep, late_other]]


def scatter_over_dp(ql, kl, qg, kg, qh, kh, qp, kp, q_rows, k_rows, width):
    count = lax.axis_size("dp")
    head_count = count // 2
    terms = []
    for latent, grad, rows in ((ql, qg, q_rows), (kl, kg, k_rows)):
        term = jnp.dot(latent, grad, preferred_element_type=jnp.float32)
        term = term.reshape(2, rows, head_count, width).transpose(0, 2, 1, 3)
        terms.append(term.reshape(count, rows, width))
    own = lax.psum_scatter(
        jnp.concatenate(terms, axis=1), "dp", scatter_dimension=0, tiled=True
    )[0]

    def body(qh, kh, qp, kp, rows):
        rows[...] = peak_rows(qh, kh, qp, kp, lax.axis_index("mp") * qp.shape[0])

    (rows,) = call(body, [f32(SUB, width)], qh, kh, qp, kp)
    rows = lax.pmax(rows, "dp")
    late = SUB
    return [[jnp.concatenate([own[:-late], rows], axis=0)], [own[-late:]]]


def folded(gram):
    width = gram.shape[0]
    half = width // 2
    line = lax.broadcasted_iota(jnp.int32, (half, width), 0)
    lane = lax.broadcasted_iota(jnp.int32, (half, width), 1)
    low = pltpu.roll(gram[half:, :], half, 1)
    diagonal = jnp.sum(jnp.where(line == lane, low, 0.0), axis=0, keepdims=True)
    return jnp.where((lane < half) & (line > lane), low, gram[:half, :]), diagonal


def unfolded(top, diagonal):
    half, width = top.shape
    line = lax.broadcasted_iota(jnp.int32, (half, width), 0)
    lane = lax.broadcasted_iota(jnp.int32, (half, width), 1)
    turned = jnp.transpose(jnp.concatenate([top, jnp.zeros_like(top)], axis=0))
    over = turned[:half, :]
    low = jnp.where(line > lane, top, jnp.where(line == lane, diagonal, over))
    above = jnp.where((lane < half) & (line > lane), over, top)
    below = jnp.where(lane < half, turned[half:, :], pltpu.roll(low, half, 1))
    return jnp.concatenate([above, below], axis=0)


def gather_body(*refs):
    *parts, out = refs
    top = parts[0].shape[0] - SUB
    total, high = parts[0][...], parts[0][top:, :]
    for part in parts[1:]:
        total = total + part[...]
        high = jnp.maximum(high, part[top:, :])
    line = lax.broadcasted_iota(jnp.int32, high.shape, 0)
    out[:top, :] = total[:top, :]
    out[top:, :] = jnp.where(line < 1, total[top:, :], high)


def gram_body(*refs, groups, q_rows):
    mq, mk = refs[0], refs[1]
    mq_new, mk_new, keep, send = refs[-4:]
    own, start = [], 2
    for n, size in enumerate(groups):
        parts = refs[start : start + size]
        start += size
        share = parts[0].shape[0] - (0 if n else SUB)
        total = parts[0][:share, :]
        for part in parts[1:]:
            total = total + part[:share, :]
        own.append(total)
        if not n:
            rows = parts[0][share:, :]
            for part in parts[1:]:
                if part.shape[0] > share:
                    rows = jnp.maximum(rows, part[share:, :])
    own = jnp.concatenate(own, axis=0)
    q = MOMENTUM * mq[...] + own[:q_rows]
    k = MOMENTUM * mk[...] + own[q_rows:]
    mq_new[...] = q
    mk_new[...] = k
    q_gram = product(q, q, ((0,), (0,)))
    k_gram = product(k, k, ((0,), (0,)))
    half = q_gram.shape[0] // 2
    odd = lax.axis_index("mp") % 2 == 1
    q_top, q_rest = folded(q_gram)
    k_top, k_rest = folded(k_gram)
    line = lax.broadcasted_iota(jnp.int32, rows.shape, 0)
    keep[:half, :] = jnp.where(odd, k_top, q_top)
    send[:half, :] = jnp.where(odd, q_top, k_top)
    keep[half:, :] = jnp.where(line > 0, rows, jnp.where(odd, k_rest, q_rest))
    send[half:, :] = jnp.where(line > 0, rows, jnp.where(odd, q_rest, k_rest))


def finish_body(*refs, head_count, norms):
    total, other, mq, mk, wq, wk = refs[:6]
    wq_new, wk_new, mq_out, mk_out, sems = refs[6:]
    copies = [
        pltpu.make_async_copy(mq, mq_out, sems.at[0]),
        pltpu.make_async_copy(mk, mk_out, sems.at[1]),
    ]
    for copy in copies:
        copy.start()
    width = total.shape[1]
    half = width // 2
    odd = lax.axis_index("mp") % 2 == 1
    sums = [jnp.where(odd, other[...], total[...]), jnp.where(odd, total[...], other[...])]
    rows = sums[0][half:, :]
    spot = lax.broadcasted_iota(jnp.int32, rows.shape, 1)
    line = lax.broadcasted_iota(jnp.int32, rows.shape, 0)
    own = lax.axis_index("dp") % head_count
    peak = jnp.max(
        jnp.where((spot == own) & (line > 0), rows, LOW), axis=(0, 1), keepdims=True
    )
    shrink = jnp.sqrt(CLIP_LEVEL / jnp.maximum(peak, CLIP_LEVEL))
    grams = [unfolded(both[:half, :], both[half : half + 1, :]) for both in sums]
    line = lax.broadcasted_iota(jnp.int32, (width, width), 0)
    diagonal = line == lax.broadcasted_iota(jnp.int32, (width, width), 1)
    unit = jnp.where(diagonal, COEFF_A, 0.0)
    moved = [left(pieces(value[...])) for value in (mq, mk)]
    scales, shrunk = [], []
    for gram in grams:
        trace = jnp.sum(jnp.where(diagonal, gram, 0.0), axis=(0, 1), keepdims=True)
        scales.append(1.0 / jnp.sqrt(trace + 1.0))
        shrunk.append(scales[-1] * scales[-1])
    both = range(2)
    for step in range(ITERS):
        factors = [1.0, 1.0] if step else shrunk
        parts = [pieces(gram) for gram in grams]
        bases = [right(part) for part in parts]
        squares = [stacked(left(parts[n]), bases[n]) for n in both]
        splits = [
            pieces(
                unit
                + factors[n] * (COEFF_B * grams[n] + (COEFF_C * factors[n]) * squares[n])
            )
            for n in both
        ]
        follows = [right(split) for split in splits]
        last = step + 1 == ITERS
        if not last:
            inner = [stacked(left(splits[n]), bases[n]) * factors[n] for n in both]
            grams = [stacked(left(pieces(inner[n])), follows[n]) for n in both]
        moved = [stacked(moved[n], follows[n]) for n in both]
        if not last:
            moved = [left(pieces(value)) for value in moved]
    keep = 1.0 - STEP_SIZE * DECAY
    for n, (weight, out) in enumerate(((wq, wq_new), (wk, wk_new))):
        out[...] = (weight[...] * keep - (norms[n] * scales[n]) * moved[n]) * shrink
    for copy in copies:
        copy.wait()


def local(
    q_latent,
    kv_latent,
    q_head_grad,
    k_head_grad,
    q_heads,
    k_heads,
    query_pick,
    key_pick,
    q_weight,
    k_weight,
    q_moment,
    k_moment,
):
    dp, mp = lax.axis_size("dp"), lax.axis_size("mp")
    head_count = dp // 2
    tokens = q_latent.shape[0]
    q_rows, k_rows = q_latent.shape[2], kv_latent.shape[2]
    width = q_moment.shape[2]
    ql = jnp.transpose(q_latent, (1, 2, 0)).reshape(2 * q_rows, tokens)
    kl = jnp.transpose(kv_latent, (1, 2, 0)).reshape(2 * k_rows, tokens)
    qp = jnp.transpose(query_pick[0], (1, 0))
    kp = jnp.transpose(key_pick[0], (1, 0))
    direct = dp <= 16 and dp & (dp - 1) == 0
    reduce = sum_over_dp if direct else scatter_over_dp
    groups = reduce(
        ql, kl, q_head_grad, k_head_grad, q_heads, k_heads, qp, kp, q_rows, k_rows, width
    )
    mq, mk, keep, send = call(
        functools.partial(gram_body, groups=[len(group) for group in groups], q_rows=q_rows),
        [f32(q_rows, width), f32(k_rows, width)] + [f32(width // 2 + SUB, width)] * 2,
        q_moment[0], k_moment[0], *sum(groups, []),
    )
    pair = [(core, core ^ 1) for core in range(mp)]
    other = lax.ppermute(send, "mp", pair)
    (joined,) = call(gather_body, [f32(width // 2 + SUB, width)], keep, other)
    parts = [joined]
    for far in (1, 0):
        for near in range(mp // 2):
            if far or near:
                route = [
                    (d * mp + m, (d + far * head_count) % dp * mp + (m + 2 * near) % mp)
                    for d in range(dp)
                    for m in range(mp)
                ]
                parts.append(lax.ppermute(joined, ("dp", "mp"), route))
    (total,) = call(gather_body, [f32(width // 2 + SUB, width)], *parts)
    back = lax.ppermute(total, "mp", pair)
    norms = [STEP_SIZE * 0.2 * math.sqrt(2 * rows * mp) for rows in (q_rows, k_rows)]
    wq_new, wk_new, mq_new, mk_new = call(
        functools.partial(finish_body, head_count=head_count, norms=norms),
        [f32(q_rows, width), f32(k_rows, width)]
        + [pltpu.HBM(value.shape, jnp.float32) for value in (mq, mk)],
        total, back, mq, mk, q_weight[0], k_weight[0],
        scratch=[pltpu.SemaphoreType.DMA((2,))],
    )
    return (wq_new[None], wk_new[None], mq_new[None], mk_new[None])


def solution(mesh):
    in_specs = (
        P("dp", None, "mp"),
        P("dp", None, "mp"),
        P("dp", None),
        P("dp", None),
        P("dp", "mp"),
        P("dp", "mp"),
        P("dp", None, "mp"),
        P("dp", None, "mp"),
        P("dp", "mp", None),
        P("dp", "mp", None),
        P("dp", "mp", None),
        P("dp", "mp", None),
    )
    out_specs = (P("dp", "mp", None), P("dp", "mp", None), P("dp", "mp", None), P("dp", "mp", None))

    return jax.shard_map(local, mesh=mesh, in_specs=in_specs, out_specs=out_specs, check_vma=False)
```

```python
import functools
import math

import jax
import jax.numpy as jnp
from jax import lax
from jax.experimental import pallas as pl
from jax.experimental.pallas import tpu as pltpu
from jax.sharding import PartitionSpec as P


ITERS = 5
MOMENTUM = 0.95
STEP_SIZE = 1.0
DECAY = 0.1
CLIP_LEVEL = 0.1
SCORE_SCALE = 1.0 / math.sqrt(192.0)
COEFF_A = 3.4445
COEFF_B = -4.775
COEFF_C = 2.0315
HIGHEST = lax.Precision.HIGHEST
SUB = 8
LANES = 128
LOW = -1e30
FIRST_SHARES = (0.625,)


VMEM = pl.BlockSpec(memory_space=pltpu.VMEM)
ANY = pl.BlockSpec(memory_space=pl.ANY)


def f32(*shape):
    return jax.ShapeDtypeStruct(shape, jnp.float32)


def call(body, outs, *args, scratch=(), limit=4, fetched=False):
    if fetched:
        args = [pltpu.with_memory_space_constraint(arg, pltpu.HBM) for arg in args]
    return pl.pallas_call(
        body,
        out_shape=outs,
        in_specs=[ANY if fetched else VMEM] * len(args),
        out_specs=[VMEM if isinstance(out, jax.ShapeDtypeStruct) else ANY for out in outs],
        scratch_shapes=scratch,
        compiler_params=pltpu.CompilerParams(vmem_limit_bytes=limit * 2**20),
    )(*args)


def product(x, y, dims):
    return lax.dot_general(
        x, y, (dims, ((), ())), precision=HIGHEST, preferred_element_type=jnp.float32
    )


def pieces(x):
    high = x.astype(jnp.bfloat16)
    rest = x - high.astype(jnp.float32)
    middle = rest.astype(jnp.bfloat16)
    return high, middle, (rest - middle.astype(jnp.float32)).astype(jnp.bfloat16)


def left(x):
    high, middle, low = x
    return jnp.concatenate([high, middle], axis=1), jnp.concatenate([high, low], axis=1)


def right(x):
    high, middle, low = x
    pair = jnp.concatenate([high, middle], axis=1)
    return jnp.concatenate([pair, pair], axis=0), jnp.concatenate([low, high], axis=0)


def stacked(x, y):
    four = jnp.dot(x[0], y[0], preferred_element_type=jnp.float32)
    two = jnp.dot(x[1], y[1], preferred_element_type=jnp.float32)
    width = two.shape[1]
    return four[:, :width] + (four[:, width:] + two)


def peak_rows(q_heads, k_heads, query_pick, key_pick, first_head):
    tokens = q_heads.shape[0]
    heads, picks = query_pick.shape
    width = q_heads.shape[1] // heads
    spot = lax.broadcasted_iota(jnp.int32, (SUB, LANES), 1)
    token = lax.broadcasted_iota(jnp.int32, (tokens, picks), 0)
    rows = jnp.full((SUB, LANES), LOW, jnp.float32)
    for head in range(heads):
        picked = []
        for pick, held in ((query_pick, q_heads), (key_pick, k_heads)):
            chosen = (token == pick[head : head + 1, :]).astype(jnp.float32).astype(jnp.bfloat16)
            values = held[:, head * width : (head + 1) * width]
            picked.append(
                lax.dot_general(
                    chosen, values, (((0,), (0,)), ((), ())), preferred_element_type=jnp.float32
                )
            )
        scores = jnp.sum(picked[0] * picked[1], axis=1, keepdims=True) * SCORE_SCALE
        top = jnp.max(scores, axis=0, keepdims=True)
        rows = jnp.where(spot == first_head + head, top, rows)
    return rows


def terms_body(*refs, head_count, q_rows, k_rows, shares, width):
    sources, held = refs[:8], refs[-10:]
    xs = refs[8 : 8 + len(shares)]
    ka = refs[8 + len(shares) : 8 + 2 * len(shares)]
    zb = refs[8 + 2 * len(shares) : -10]
    ql, kl, qg, kg, qh, kh, qp, kp, tiles, sems = held
    copies = [
        pltpu.make_async_copy(source, kept, sems.at[n])
        for n, (source, kept) in enumerate(zip(sources, held[:8]))
    ]
    for n in (0, 2, 1, 3, 4, 5, 6, 7):
        copies[n].start()
    device = lax.axis_index("dp")
    for latent, grad, rows, start, n in ((ql, qg, q_rows, 0, 0), (kl, kg, k_rows, q_rows, 1)):
        copies[n].wait()
        copies[n + 2].wait()
        for half in range(2):
            term = jnp.dot(
                latent[half * rows : (half + 1) * rows, :],
                grad[...],
                preferred_element_type=jnp.float32,
            )
            for head in range(head_count):
                tiles[half * head_count + head, start : start + rows, :] = term[
                    :, head * width : (head + 1) * width
                ]
    row_count = q_rows + k_rows
    late = row_count - sum(shares)
    for step in range(2 * head_count):
        tile = tiles[device ^ step]
        outer, inner = step // 2, step % 2
        start = 0
        for out, share in zip(xs if inner else ka, shares):
            out[outer * share : (outer + 1) * share, :] = tile[start : start + share]
            start += share
        zb[outer][inner * late : (inner + 1) * late, :] = tile[start:]
    for copy in copies[4:]:
        copy.wait()
    rows = peak_rows(qh, kh, qp, kp, lax.axis_index("mp") * qp.shape[0])
    xs[0][head_count * shares[0] :, :] = rows
    ka[0][head_count * shares[0] :, :] = rows


def inner_sum_body(ka, rx, *outs):
    count = len(outs)
    share = ka.shape[0] // count // SUB * SUB
    for step, out in enumerate(outs):
        part = slice(step * share, (step + 1) * share)
        out[:share, :] = ka[part, :] + rx[part, :]
        if out.shape[0] > share:
            out[share:, :] = jnp.maximum(ka[count * share :, :], rx[count * share :, :])


def outer_sum_body(*refs):
    *parts, keep, send = refs
    late = keep.shape[0]
    total = parts[0][...]
    for part in parts[1:]:
        total = total + part[...]
    keep[...] = total[:late]
    send[...] = total[late:]


def sum_over_dp(ql, kl, qg, kg, qh, kh, qp, kp, q_rows, k_rows, width):
    count = lax.axis_size("dp")
    head_count = count // 2
    row_count = q_rows + k_rows
    shares = [int(row_count * share) // SUB * SUB for share in FIRST_SHARES]
    extra = [SUB] + [0] * (len(shares) - 1)
    late = row_count - sum(shares)
    body = functools.partial(
        terms_body,
        head_count=head_count,
        q_rows=q_rows,
        k_rows=k_rows,
        shares=shares,
        width=width,
    )
    firsts = [f32(head_count * share + more, width) for share, more in zip(shares, extra)]
    args = (ql, kl, qg, kg, qh, kh, qp, kp)
    made = call(
        body,
        firsts + firsts + [f32(2 * late, width)] * head_count,
        *args,
        scratch=[pltpu.VMEM(arg.shape, arg.dtype) for arg in args]
        + [pltpu.VMEM((count, row_count, width), jnp.float32), pltpu.SemaphoreType.DMA((8,))],
        limit=12,
        fetched=True,
    )
    xs, ka, zb = made[: len(shares)], made[len(shares) : 2 * len(shares)], made[2 * len(shares) :]
    across = [(source, source ^ 1) for source in range(count)]
    steps = list(range(2, head_count)) + [1]

    def along(value, step):
        route = [(source, source ^ (2 * step)) for source in range(count)]
        return lax.ppermute(value, "dp", route)

    rx = [lax.ppermute(value, "dp", across) for value in xs]
    rz = [along(zb[step], step) for step in steps]
    firsts = []
    for n, (share, more) in enumerate(zip(shares, extra)):
        rides = [more if step <= (head_count - 1) // 2 else 0 for step in range(head_count)]
        sums = call(
            inner_sum_body,
            [f32(share + ride, width) for ride in rides],
            ka[n], rx[n],
        )
        firsts.append([sums[0]] + [along(sums[step], step) for step in steps])
    late_keep, late_send = call(outer_sum_body, [f32(late, width)] * 2, zb[0], *rz)
    late_other = lax.ppermute(late_send, "dp", across)
    return [*firsts, [late_keep, late_other]]


def scatter_over_dp(ql, kl, qg, kg, qh, kh, qp, kp, q_rows, k_rows, width):
    count = lax.axis_size("dp")
    head_count = count // 2
    terms = []
    for latent, grad, rows in ((ql, qg, q_rows), (kl, kg, k_rows)):
        term = jnp.dot(latent, grad, preferred_element_type=jnp.float32)
        term = term.reshape(2, rows, head_count, width).transpose(0, 2, 1, 3)
        terms.append(term.reshape(count, rows, width))
    own = lax.psum_scatter(
        jnp.concatenate(terms, axis=1), "dp", scatter_dimension=0, tiled=True
    )[0]

    def body(qh, kh, qp, kp, rows):
        rows[...] = peak_rows(qh, kh, qp, kp, lax.axis_index("mp") * qp.shape[0])

    (rows,) = call(body, [f32(SUB, width)], qh, kh, qp, kp)
    rows = lax.pmax(rows, "dp")
    late = SUB
    return [[jnp.concatenate([own[:-late], rows], axis=0)], [own[-late:]]]


def folded(gram):
    width = gram.shape[0]
    half = width // 2
    line = lax.broadcasted_iota(jnp.int32, (half, width), 0)
    lane = lax.broadcasted_iota(jnp.int32, (half, width), 1)
    low = pltpu.roll(gram[half:, :], half, 1)
    diagonal = jnp.sum(jnp.where(line == lane, low, 0.0), axis=0, keepdims=True)
    return jnp.where((lane < half) & (line > lane), low, gram[:half, :]), diagonal


def unfolded(top, diagonal):
    half, width = top.shape
    line = lax.broadcasted_iota(jnp.int32, (half, width), 0)
    lane = lax.broadcasted_iota(jnp.int32, (half, width), 1)
    turned = jnp.transpose(jnp.concatenate([top, jnp.zeros_like(top)], axis=0))
    over = turned[:half, :]
    low = jnp.where(line > lane, top, jnp.where(line == lane, diagonal, over))
    above = jnp.where((lane < half) & (line > lane), over, top)
    below = jnp.where(lane < half, turned[half:, :], pltpu.roll(low, half, 1))
    return jnp.concatenate([above, below], axis=0)


def gathered(parts):
    top = parts[0].shape[0] - SUB
    total, high = parts[0], parts[0][top:, :]
    for part in parts[1:]:
        total = total + part
        high = jnp.maximum(high, part[top:, :])
    line = lax.broadcasted_iota(jnp.int32, high.shape, 0)
    return jnp.concatenate([total[:top, :], jnp.where(line < 2, total[top:, :], high)], axis=0)


def join_body(pack, given, out):
    out[...] = gathered([pack[...], given[...]])


def total_body(joined, *refs):
    *parts, out = refs
    parts = [part[...] for part in parts]

    @pl.when(lax.axis_index("mp") % 2 == 1)
    def _():
        out[...] = gathered([joined[...], *parts])

    @pl.when(lax.axis_index("mp") % 2 == 0)
    def _():
        if len(parts) > 1:
            out[...] = gathered(parts[:-1])
        else:
            line = lax.broadcasted_iota(jnp.int32, out.shape, 0)
            out[...] = jnp.where(line < out.shape[0] - SUB + 2, 0.0, LOW)


def gram_body(*refs, groups, q_rows):
    mq, mk = refs[0], refs[1]
    mq_new, mk_new, pack = refs[-3:]
    own, start = [], 2
    for n, size in enumerate(groups):
        parts = refs[start : start + size]
        start += size
        share = parts[0].shape[0] - (0 if n else SUB)
        total = parts[0][:share, :]
        for part in parts[1:]:
            total = total + part[:share, :]
        own.append(total)
        if not n:
            rows = parts[0][share:, :]
            for part in parts[1:]:
                if part.shape[0] > share:
                    rows = jnp.maximum(rows, part[share:, :])
    own = jnp.concatenate(own, axis=0)
    q = MOMENTUM * mq[...] + own[:q_rows]
    k = MOMENTUM * mk[...] + own[q_rows:]
    mq_new[...] = q
    mk_new[...] = k
    q_gram = product(q, q, ((0,), (0,)))
    k_gram = product(k, k, ((0,), (0,)))
    half = q_gram.shape[0] // 2
    pack[:half, :], q_rest = folded(q_gram)
    pack[half : 2 * half, :], k_rest = folded(k_gram)
    line = lax.broadcasted_iota(jnp.int32, rows.shape, 0)
    pack[2 * half :, :] = jnp.where(line == 0, q_rest, jnp.where(line == 1, k_rest, rows))


def finish_body(*refs, head_count, norms):
    total, other, mq, mk, wq, wk = refs[:6]
    wq_new, wk_new, mq_out, mk_out, sems = refs[6:]
    copies = [
        pltpu.make_async_copy(mq, mq_out, sems.at[0]),
        pltpu.make_async_copy(mk, mk_out, sems.at[1]),
    ]
    for copy in copies:
        copy.start()
    merged = gathered([total[...], other[...]])
    width = total.shape[1]
    half = width // 2
    rows = merged[2 * half :, :]
    spot = lax.broadcasted_iota(jnp.int32, rows.shape, 1)
    line = lax.broadcasted_iota(jnp.int32, rows.shape, 0)
    own = lax.axis_index("dp") % head_count
    peak = jnp.max(
        jnp.where((spot == own) & (line > 1), rows, LOW), axis=(0, 1), keepdims=True
    )
    shrink = jnp.sqrt(CLIP_LEVEL / jnp.maximum(peak, CLIP_LEVEL))
    grams = [
        unfolded(merged[n * half : (n + 1) * half, :], rows[n : n + 1, :]) for n in range(2)
    ]
    line = lax.broadcasted_iota(jnp.int32, (width, width), 0)
    diagonal = line == lax.broadcasted_iota(jnp.int32, (width, width), 1)
    unit = jnp.where(diagonal, COEFF_A, 0.0)
    moved = [left(pieces(value[...])) for value in (mq, mk)]
    scales, shrunk = [], []
    for gram in grams:
        trace = jnp.sum(jnp.where(diagonal, gram, 0.0), axis=(0, 1), keepdims=True)
        scales.append(1.0 / jnp.sqrt(trace + 1.0))
        shrunk.append(scales[-1] * scales[-1])
    both = range(2)
    for step in range(ITERS):
        factors = [1.0, 1.0] if step else shrunk
        parts = [pieces(gram) for gram in grams]
        bases = [right(part) for part in parts]
        squares = [stacked(left(parts[n]), bases[n]) for n in both]
        splits = [
            pieces(
                unit
                + factors[n] * (COEFF_B * grams[n] + (COEFF_C * factors[n]) * squares[n])
            )
            for n in both
        ]
        follows = [right(split) for split in splits]
        last = step + 1 == ITERS
        if not last:
            inner = [stacked(left(splits[n]), bases[n]) * factors[n] for n in both]
            grams = [stacked(left(pieces(inner[n])), follows[n]) for n in both]
        moved = [stacked(moved[n], follows[n]) for n in both]
        if not last:
            moved = [left(pieces(value)) for value in moved]
    keep = 1.0 - STEP_SIZE * DECAY
    for n, (weight, out) in enumerate(((wq, wq_new), (wk, wk_new))):
        out[...] = (weight[...] * keep - (norms[n] * scales[n]) * moved[n]) * shrink
    for copy in copies:
        copy.wait()


def local(
    q_latent,
    kv_latent,
    q_head_grad,
    k_head_grad,
    q_heads,
    k_heads,
    query_pick,
    key_pick,
    q_weight,
    k_weight,
    q_moment,
    k_moment,
):
    dp, mp = lax.axis_size("dp"), lax.axis_size("mp")
    head_count = dp // 2
    tokens = q_latent.shape[0]
    q_rows, k_rows = q_latent.shape[2], kv_latent.shape[2]
    width = q_moment.shape[2]
    ql = jnp.transpose(q_latent, (1, 2, 0)).reshape(2 * q_rows, tokens)
    kl = jnp.transpose(kv_latent, (1, 2, 0)).reshape(2 * k_rows, tokens)
    qp = jnp.transpose(query_pick[0], (1, 0))
    kp = jnp.transpose(key_pick[0], (1, 0))
    direct = dp <= 16 and dp & (dp - 1) == 0
    reduce = sum_over_dp if direct else scatter_over_dp
    groups = reduce(
        ql, kl, q_head_grad, k_head_grad, q_heads, k_heads, qp, kp, q_rows, k_rows, width
    )
    folded_pair = f32(width + SUB, width)
    mq, mk, pack = call(
        functools.partial(gram_body, groups=[len(group) for group in groups], q_rows=q_rows),
        [f32(q_rows, width), f32(k_rows, width), folded_pair],
        q_moment[0], k_moment[0], *sum(groups, []),
    )
    pair = [(core, core ^ 1) for core in range(mp)]
    given = lax.ppermute(pack, "mp", pair)
    (joined,) = call(join_body, [folded_pair], pack, given)
    peers = [(1, near) for near in reversed(range(mp // 2))]
    peers += [(0, near) for near in range(1, mp // 2)]
    parts = []
    for n in range(mp // 2):
        shifts = [peers[2 * n + 1] if 2 * n + 1 < len(peers) else (0, 0), peers[2 * n]]
        route = []
        for d in range(dp):
            for m in range(mp):
                far, near = shifts[m % 2]
                route.append(
                    (d * mp + m, (d + far * head_count) % dp * mp + (m + 2 * near) % mp)
                )
        parts.append(lax.ppermute(joined, ("dp", "mp"), route))
    (total,) = call(total_body, [folded_pair], joined, *parts)
    back = lax.ppermute(total, "mp", pair)
    norms = [STEP_SIZE * 0.2 * math.sqrt(2 * rows * mp) for rows in (q_rows, k_rows)]
    wq_new, wk_new, mq_new, mk_new = call(
        functools.partial(finish_body, head_count=head_count, norms=norms),
        [f32(q_rows, width), f32(k_rows, width)]
        + [pltpu.HBM(value.shape, jnp.float32) for value in (mq, mk)],
        total, back, mq, mk, q_weight[0], k_weight[0],
        scratch=[pltpu.SemaphoreType.DMA((2,))],
    )
    return (wq_new[None], wk_new[None], mq_new[None], mk_new[None])


def solution(mesh):
    in_specs = (
        P("dp", None, "mp"),
        P("dp", None, "mp"),
        P("dp", None),
        P("dp", None),
        P("dp", "mp"),
        P("dp", "mp"),
        P("dp", None, "mp"),
        P("dp", None, "mp"),
        P("dp", "mp", None),
        P("dp", "mp", None),
        P("dp", "mp", None),
        P("dp", "mp", None),
    )
    out_specs = (P("dp", "mp", None), P("dp", "mp", None), P("dp", "mp", None), P("dp", "mp", None))

    return jax.shard_map(local, mesh=mesh, in_specs=in_specs, out_specs=out_specs, check_vma=False)
```

```python
import functools
import math

import jax
import jax.numpy as jnp
from jax import lax
from jax.experimental import pallas as pl
from jax.experimental.pallas import tpu as pltpu
from jax.sharding import PartitionSpec as P


ITERS = 5
MOMENTUM = 0.95
STEP_SIZE = 1.0
DECAY = 0.1
CLIP_LEVEL = 0.1
SCORE_SCALE = 1.0 / math.sqrt(192.0)
COEFF_A = 3.4445
COEFF_B = -4.775
COEFF_C = 2.0315
HIGHEST = lax.Precision.HIGHEST
SUB = 8
LANES = 128
LOW = -1e30
FIRST_SHARES = (0.625,)


VMEM = pl.BlockSpec(memory_space=pltpu.VMEM)
ANY = pl.BlockSpec(memory_space=pl.ANY)


def f32(*shape):
    return jax.ShapeDtypeStruct(shape, jnp.float32)


def call(body, outs, *args, scratch=(), limit=4, fetched=False):
    if fetched:
        args = [pltpu.with_memory_space_constraint(arg, pltpu.HBM) for arg in args]
    return pl.pallas_call(
        body,
        out_shape=outs,
        in_specs=[ANY if fetched else VMEM] * len(args),
        out_specs=[VMEM if isinstance(out, jax.ShapeDtypeStruct) else ANY for out in outs],
        scratch_shapes=scratch,
        compiler_params=pltpu.CompilerParams(vmem_limit_bytes=limit * 2**20),
    )(*args)


def product(x, y, dims):
    return lax.dot_general(
        x, y, (dims, ((), ())), precision=HIGHEST, preferred_element_type=jnp.float32
    )


def pieces(x):
    high = x.astype(jnp.bfloat16)
    rest = x - high.astype(jnp.float32)
    middle = rest.astype(jnp.bfloat16)
    return high, middle, (rest - middle.astype(jnp.float32)).astype(jnp.bfloat16)


def left(x):
    high, middle, low = x
    return jnp.concatenate([high, middle], axis=1), jnp.concatenate([high, low], axis=1)


def right(x):
    high, middle, low = x
    pair = jnp.concatenate([high, middle], axis=1)
    return jnp.concatenate([pair, pair], axis=0), jnp.concatenate([low, high], axis=0)


def stacked(x, y):
    four = jnp.dot(x[0], y[0], preferred_element_type=jnp.float32)
    two = jnp.dot(x[1], y[1], preferred_element_type=jnp.float32)
    width = two.shape[1]
    return four[:, :width] + (four[:, width:] + two)


def peak_rows(q_heads, k_heads, query_pick, key_pick, first_head):
    tokens = q_heads.shape[0]
    heads, picks = query_pick.shape
    width = q_heads.shape[1] // heads
    spot = lax.broadcasted_iota(jnp.int32, (SUB, LANES), 1)
    token = lax.broadcasted_iota(jnp.int32, (tokens, picks), 0)
    rows = jnp.full((SUB, LANES), LOW, jnp.float32)
    for head in range(heads):
        picked = []
        for pick, held in ((query_pick, q_heads), (key_pick, k_heads)):
            chosen = (token == pick[head : head + 1, :]).astype(jnp.float32).astype(jnp.bfloat16)
            values = held[:, head * width : (head + 1) * width]
            picked.append(
                lax.dot_general(
                    chosen, values, (((0,), (0,)), ((), ())), preferred_element_type=jnp.float32
                )
            )
        scores = jnp.sum(picked[0] * picked[1], axis=1, keepdims=True) * SCORE_SCALE
        top = jnp.max(scores, axis=0, keepdims=True)
        rows = jnp.where(spot == first_head + head, top, rows)
    return rows


def terms_body(*refs, head_count, q_rows, k_rows, shares, width):
    sources, held = refs[:8], refs[-10:]
    xs = refs[8 : 8 + len(shares)]
    ka = refs[8 + len(shares) : 8 + 2 * len(shares)]
    zb = refs[8 + 2 * len(shares) : -10]
    ql, kl, qg, kg, qh, kh, qp, kp, tiles, sems = held
    copies = [
        pltpu.make_async_copy(source, kept, sems.at[n])
        for n, (source, kept) in enumerate(zip(sources, held[:8]))
    ]
    for n in (0, 2, 1, 3, 4, 5, 6, 7):
        copies[n].start()
    device = lax.axis_index("dp")
    for latent, grad, rows, start, n in ((ql, qg, q_rows, 0, 0), (kl, kg, k_rows, q_rows, 1)):
        copies[n].wait()
        copies[n + 2].wait()
        for half in range(2):
            term = jnp.dot(
                latent[half * rows : (half + 1) * rows, :],
                grad[...],
                preferred_element_type=jnp.float32,
            )
            for head in range(head_count):
                tiles[half * head_count + head, start : start + rows, :] = term[
                    :, head * width : (head + 1) * width
                ]
    row_count = q_rows + k_rows
    late = row_count - sum(shares)
    for step in range(2 * head_count):
        tile = tiles[device ^ step]
        outer, inner = step // 2, step % 2
        start = 0
        for out, share in zip(xs if inner else ka, shares):
            out[outer * share : (outer + 1) * share, :] = tile[start : start + share]
            start += share
        zb[outer][inner * late : (inner + 1) * late, :] = tile[start:]
    for copy in copies[4:]:
        copy.wait()
    rows = peak_rows(qh, kh, qp, kp, lax.axis_index("mp") * qp.shape[0])
    xs[0][head_count * shares[0] :, :] = rows
    ka[0][head_count * shares[0] :, :] = rows


def inner_sum_body(ka, rx, *outs):
    count = len(outs)
    share = ka.shape[0] // count // SUB * SUB
    for step, out in enumerate(outs):
        part = slice(step * share, (step + 1) * share)
        out[:share, :] = ka[part, :] + rx[part, :]
        if out.shape[0] > share:
            out[share:, :] = jnp.maximum(ka[count * share :, :], rx[count * share :, :])


def outer_sum_body(*refs):
    *parts, keep, send = refs
    late = keep.shape[0]
    total = parts[0][...]
    for part in parts[1:]:
        total = total + part[...]
    keep[...] = total[:late]
    send[...] = total[late:]


def sum_over_dp(ql, kl, qg, kg, qh, kh, qp, kp, q_rows, k_rows, width):
    count = lax.axis_size("dp")
    head_count = count // 2
    row_count = q_rows + k_rows
    shares = [int(row_count * share) // SUB * SUB for share in FIRST_SHARES]
    extra = [SUB] + [0] * (len(shares) - 1)
    late = row_count - sum(shares)
    body = functools.partial(
        terms_body,
        head_count=head_count,
        q_rows=q_rows,
        k_rows=k_rows,
        shares=shares,
        width=width,
    )
    firsts = [f32(head_count * share + more, width) for share, more in zip(shares, extra)]
    args = (ql, kl, qg, kg, qh, kh, qp, kp)
    made = call(
        body,
        firsts + firsts + [f32(2 * late, width)] * head_count,
        *args,
        scratch=[pltpu.VMEM(arg.shape, arg.dtype) for arg in args]
        + [pltpu.VMEM((count, row_count, width), jnp.float32), pltpu.SemaphoreType.DMA((8,))],
        limit=12,
        fetched=True,
    )
    xs, ka, zb = made[: len(shares)], made[len(shares) : 2 * len(shares)], made[2 * len(shares) :]
    across = [(source, source ^ 1) for source in range(count)]
    steps = list(range(2, head_count)) + [1]

    def along(value, step):
        route = [(source, source ^ (2 * step)) for source in range(count)]
        return lax.ppermute(value, "dp", route)

    rx = [lax.ppermute(value, "dp", across) for value in xs]
    rz = [along(zb[step], step) for step in steps]
    firsts = []
    for n, (share, more) in enumerate(zip(shares, extra)):
        rides = [more if step <= (head_count - 1) // 2 else 0 for step in range(head_count)]
        sums = call(
            inner_sum_body,
            [f32(share + ride, width) for ride in rides],
            ka[n], rx[n],
        )
        firsts.append([sums[0]] + [along(sums[step], step) for step in steps])
    late_keep, late_send = call(outer_sum_body, [f32(late, width)] * 2, zb[0], *rz)
    late_other = lax.ppermute(late_send, "dp", across)
    return [*firsts, [late_keep, late_other]]


def scatter_over_dp(ql, kl, qg, kg, qh, kh, qp, kp, q_rows, k_rows, width):
    count = lax.axis_size("dp")
    head_count = count // 2
    terms = []
    for latent, grad, rows in ((ql, qg, q_rows), (kl, kg, k_rows)):
        term = jnp.dot(latent, grad, preferred_element_type=jnp.float32)
        term = term.reshape(2, rows, head_count, width).transpose(0, 2, 1, 3)
        terms.append(term.reshape(count, rows, width))
    own = lax.psum_scatter(
        jnp.concatenate(terms, axis=1), "dp", scatter_dimension=0, tiled=True
    )[0]

    def body(qh, kh, qp, kp, rows):
        rows[...] = peak_rows(qh, kh, qp, kp, lax.axis_index("mp") * qp.shape[0])

    (rows,) = call(body, [f32(SUB, width)], qh, kh, qp, kp)
    rows = lax.pmax(rows, "dp")
    late = SUB
    return [[jnp.concatenate([own[:-late], rows], axis=0)], [own[-late:]]]


def folded(gram):
    width = gram.shape[0]
    half = width // 2
    line = lax.broadcasted_iota(jnp.int32, (half, width), 0)
    lane = lax.broadcasted_iota(jnp.int32, (half, width), 1)
    low = pltpu.roll(gram[half:, :], half, 1)
    diagonal = jnp.sum(jnp.where(line == lane, low, 0.0), axis=0, keepdims=True)
    return jnp.where((lane < half) & (line > lane), low, gram[:half, :]), diagonal


def unfolded(top, diagonal):
    half, width = top.shape
    line = lax.broadcasted_iota(jnp.int32, (half, width), 0)
    lane = lax.broadcasted_iota(jnp.int32, (half, width), 1)
    turned = jnp.transpose(jnp.concatenate([top, jnp.zeros_like(top)], axis=0))
    over = turned[:half, :]
    low = jnp.where(line > lane, top, jnp.where(line == lane, diagonal, over))
    above = jnp.where((lane < half) & (line > lane), over, top)
    below = jnp.where(lane < half, turned[half:, :], pltpu.roll(low, half, 1))
    return jnp.concatenate([above, below], axis=0)


def gathered(parts):
    top = parts[0].shape[0] - SUB
    total, high = parts[0], parts[0][top:, :]
    for part in parts[1:]:
        total = total + part
        high = jnp.maximum(high, part[top:, :])
    line = lax.broadcasted_iota(jnp.int32, high.shape, 0)
    return jnp.concatenate([total[:top, :], jnp.where(line < 2, total[top:, :], high)], axis=0)


def join_body(pack, given, out):
    out[...] = gathered([pack[...], given[...]])


def total_body(joined, *refs):
    *parts, out = refs
    parts = [part[...] for part in parts]

    @pl.when(lax.axis_index("mp") % 2 == 1)
    def _():
        out[...] = gathered([joined[...], *parts])

    @pl.when(lax.axis_index("mp") % 2 == 0)
    def _():
        if len(parts) > 1:
            out[...] = gathered(parts[:-1])
        else:
            line = lax.broadcasted_iota(jnp.int32, out.shape, 0)
            out[...] = jnp.where(line < out.shape[0] - SUB + 2, 0.0, LOW)


def gram_body(*refs, groups, q_rows):
    mq, mk = refs[0], refs[1]
    mq_new, mk_new, pack = refs[-3:]
    own, start = [], 2
    for n, size in enumerate(groups):
        parts = refs[start : start + size]
        start += size
        share = parts[0].shape[0] - (0 if n else SUB)
        total = parts[0][:share, :]
        for part in parts[1:]:
            total = total + part[:share, :]
        own.append(total)
        if not n:
            rows = parts[0][share:, :]
            for part in parts[1:]:
                if part.shape[0] > share:
                    rows = jnp.maximum(rows, part[share:, :])
    own = jnp.concatenate(own, axis=0)
    q = MOMENTUM * mq[...] + own[:q_rows]
    k = MOMENTUM * mk[...] + own[q_rows:]
    mq_new[...] = q
    mk_new[...] = k
    q_gram = product(q, q, ((0,), (0,)))
    k_gram = product(k, k, ((0,), (0,)))
    half = q_gram.shape[0] // 2
    pack[:half, :], q_rest = folded(q_gram)
    pack[half : 2 * half, :], k_rest = folded(k_gram)
    line = lax.broadcasted_iota(jnp.int32, rows.shape, 0)
    pack[2 * half :, :] = jnp.where(line == 0, q_rest, jnp.where(line == 1, k_rest, rows))


def finish_body(*refs, head_count, norms):
    total, other, mq, mk, wq, wk = refs[:6]
    wq_new, wk_new, mq_out, mk_out, sems = refs[6:]
    copies = [
        pltpu.make_async_copy(mq, mq_out, sems.at[0]),
        pltpu.make_async_copy(mk, mk_out, sems.at[1]),
    ]
    for copy in copies:
        copy.start()
    merged = gathered([total[...], other[...]])
    width = total.shape[1]
    half = width // 2
    rows = merged[2 * half :, :]
    spot = lax.broadcasted_iota(jnp.int32, rows.shape, 1)
    line = lax.broadcasted_iota(jnp.int32, rows.shape, 0)
    own = lax.axis_index("dp") % head_count
    peak = jnp.max(
        jnp.where((spot == own) & (line > 1), rows, LOW), axis=(0, 1), keepdims=True
    )
    shrink = jnp.sqrt(CLIP_LEVEL / jnp.maximum(peak, CLIP_LEVEL))
    grams = [
        unfolded(merged[n * half : (n + 1) * half, :], rows[n : n + 1, :]) for n in range(2)
    ]
    line = lax.broadcasted_iota(jnp.int32, (width, width), 0)
    diagonal = line == lax.broadcasted_iota(jnp.int32, (width, width), 1)
    unit = jnp.where(diagonal, COEFF_A, 0.0)
    moved = [left(pieces(value[...])) for value in (mq, mk)]
    scales, shrunk = [], []
    for gram in grams:
        trace = jnp.sum(jnp.where(diagonal, gram, 0.0), axis=(0, 1), keepdims=True)
        scales.append(1.0 / jnp.sqrt(trace + 1.0))
        shrunk.append(scales[-1] * scales[-1])
    both = range(2)
    for step in range(ITERS):
        factors = [1.0, 1.0] if step else shrunk
        parts = [pieces(gram) for gram in grams]
        bases = [right(part) for part in parts]
        if step and step + 1 == ITERS:
            inner = [stacked(moved[n], bases[n]) for n in both]
            outer = [left(pieces(COEFF_B * held[n] + COEFF_C * inner[n])) for n in both]
            held = [COEFF_A * held[n] + stacked(outer[n], bases[n]) for n in both]
            break
        squares = [stacked(left(parts[n]), bases[n]) for n in both]
        splits = [
            pieces(
                unit
                + factors[n] * (COEFF_B * grams[n] + (COEFF_C * factors[n]) * squares[n])
            )
            for n in both
        ]
        follows = [right(split) for split in splits]
        if step + 1 < ITERS:
            inner = [stacked(left(splits[n]), bases[n]) * factors[n] for n in both]
            grams = [stacked(left(pieces(inner[n])), follows[n]) for n in both]
        held = [stacked(moved[n], follows[n]) for n in both]
        moved = [left(pieces(value)) for value in held]
    keep = 1.0 - STEP_SIZE * DECAY
    for n, (weight, out) in enumerate(((wq, wq_new), (wk, wk_new))):
        out[...] = (weight[...] * keep - (norms[n] * scales[n]) * held[n]) * shrink
    for copy in copies:
        copy.wait()


def local(
    q_latent,
    kv_latent,
    q_head_grad,
    k_head_grad,
    q_heads,
    k_heads,
    query_pick,
    key_pick,
    q_weight,
    k_weight,
    q_moment,
    k_moment,
):
    dp, mp = lax.axis_size("dp"), lax.axis_size("mp")
    head_count = dp // 2
    tokens = q_latent.shape[0]
    q_rows, k_rows = q_latent.shape[2], kv_latent.shape[2]
    width = q_moment.shape[2]
    ql = jnp.transpose(q_latent, (1, 2, 0)).reshape(2 * q_rows, tokens)
    kl = jnp.transpose(kv_latent, (1, 2, 0)).reshape(2 * k_rows, tokens)
    qp = jnp.transpose(query_pick[0], (1, 0))
    kp = jnp.transpose(key_pick[0], (1, 0))
    direct = dp <= 16 and dp & (dp - 1) == 0
    reduce = sum_over_dp if direct else scatter_over_dp
    groups = reduce(
        ql, kl, q_head_grad, k_head_grad, q_heads, k_heads, qp, kp, q_rows, k_rows, width
    )
    folded_pair = f32(width + SUB, width)
    mq, mk, pack = call(
        functools.partial(gram_body, groups=[len(group) for group in groups], q_rows=q_rows),
        [f32(q_rows, width), f32(k_rows, width), folded_pair],
        q_moment[0], k_moment[0], *sum(groups, []),
    )
    pair = [(core, core ^ 1) for core in range(mp)]
    given = lax.ppermute(pack, "mp", pair)
    (joined,) = call(join_body, [folded_pair], pack, given)
    peers = [(1, near) for near in reversed(range(mp // 2))]
    peers += [(0, near) for near in range(1, mp // 2)]
    parts = []
    for n in range(mp // 2):
        shifts = [peers[2 * n + 1] if 2 * n + 1 < len(peers) else (0, 0), peers[2 * n]]
        route = []
        for d in range(dp):
            for m in range(mp):
                far, near = shifts[m % 2]
                route.append(
                    (d * mp + m, (d + far * head_count) % dp * mp + (m + 2 * near) % mp)
                )
        parts.append(lax.ppermute(joined, ("dp", "mp"), route))
    (total,) = call(total_body, [folded_pair], joined, *parts)
    back = lax.ppermute(total, "mp", pair)
    norms = [STEP_SIZE * 0.2 * math.sqrt(2 * rows * mp) for rows in (q_rows, k_rows)]
    wq_new, wk_new, mq_new, mk_new = call(
        functools.partial(finish_body, head_count=head_count, norms=norms),
        [f32(q_rows, width), f32(k_rows, width)]
        + [pltpu.HBM(value.shape, jnp.float32) for value in (mq, mk)],
        total, back, mq, mk, q_weight[0], k_weight[0],
        scratch=[pltpu.SemaphoreType.DMA((2,))],
    )
    return (wq_new[None], wk_new[None], mq_new[None], mk_new[None])


def solution(mesh):
    in_specs = (
        P("dp", None, "mp"),
        P("dp", None, "mp"),
        P("dp", None),
        P("dp", None),
        P("dp", "mp"),
        P("dp", "mp"),
        P("dp", None, "mp"),
        P("dp", None, "mp"),
        P("dp", "mp", None),
        P("dp", "mp", None),
        P("dp", "mp", None),
        P("dp", "mp", None),
    )
    out_specs = (P("dp", "mp", None), P("dp", "mp", None), P("dp", "mp", None), P("dp", "mp", None))

    return jax.shard_map(local, mesh=mesh, in_specs=in_specs, out_specs=out_specs, check_vma=False)
```

```python
import functools
import math

import jax
import jax.numpy as jnp
from jax import lax
from jax.experimental import pallas as pl
from jax.experimental.pallas import tpu as pltpu
from jax.sharding import PartitionSpec as P


ITERS = 5
MOMENTUM = 0.95
STEP_SIZE = 1.0
DECAY = 0.1
CLIP_LEVEL = 0.1
SCORE_SCALE = 1.0 / math.sqrt(192.0)
COEFF_A = 3.4445
COEFF_B = -4.775
COEFF_C = 2.0315
SUB = 8
LANES = 128
LOW = -1e30
FIRST_SHARES = (0.625,)


VMEM = pl.BlockSpec(memory_space=pltpu.VMEM)
ANY = pl.BlockSpec(memory_space=pl.ANY)


def f32(*shape):
    return jax.ShapeDtypeStruct(shape, jnp.float32)


def call(body, outs, *args, scratch=(), limit=4, fetched=False):
    if fetched:
        args = [pltpu.with_memory_space_constraint(arg, pltpu.HBM) for arg in args]
    return pl.pallas_call(
        body,
        out_shape=outs,
        in_specs=[ANY if fetched else VMEM] * len(args),
        out_specs=[VMEM if isinstance(out, jax.ShapeDtypeStruct) else ANY for out in outs],
        scratch_shapes=scratch,
        compiler_params=pltpu.CompilerParams(vmem_limit_bytes=limit * 2**20),
    )(*args)


def pieces(x):
    high = x.astype(jnp.bfloat16)
    rest = x - high.astype(jnp.float32)
    middle = rest.astype(jnp.bfloat16)
    return high, middle, (rest - middle.astype(jnp.float32)).astype(jnp.bfloat16)


def left(x):
    high, middle, low = x
    return jnp.concatenate([high, middle], axis=1), jnp.concatenate([high, low], axis=1)


def right(x):
    high, middle, low = x
    pair = jnp.concatenate([high, middle], axis=1)
    return jnp.concatenate([pair, pair], axis=0), jnp.concatenate([low, high], axis=0)


def stacked(x, y):
    four = jnp.dot(x[0], y[0], preferred_element_type=jnp.float32)
    two = jnp.dot(x[1], y[1], preferred_element_type=jnp.float32)
    width = two.shape[1]
    return four[:, :width] + (four[:, width:] + two)


def own_gram(x):
    high, middle, low = pieces(x)
    pair = jnp.concatenate([high, middle], axis=1)
    dims = (((0,), (0,)), ((), ()))
    four = lax.dot_general(
        jnp.concatenate([high, middle], axis=0),
        jnp.concatenate([pair, pair], axis=0),
        dims,
        preferred_element_type=jnp.float32,
    )
    two = lax.dot_general(
        jnp.concatenate([high, low], axis=0),
        jnp.concatenate([low, high], axis=0),
        dims,
        preferred_element_type=jnp.float32,
    )
    width = two.shape[1]
    return four[:, :width] + (four[:, width:] + two)


def peak_rows(q_heads, k_heads, query_pick, key_pick, first_head):
    tokens = q_heads.shape[0]
    heads, picks = query_pick.shape
    width = q_heads.shape[1] // heads
    spot = lax.broadcasted_iota(jnp.int32, (SUB, LANES), 1)
    token = lax.broadcasted_iota(jnp.int32, (tokens, picks), 0)
    rows = jnp.full((SUB, LANES), LOW, jnp.float32)
    for head in range(heads):
        picked = []
        for pick, held in ((query_pick, q_heads), (key_pick, k_heads)):
            chosen = (token == pick[head : head + 1, :]).astype(jnp.float32).astype(jnp.bfloat16)
            values = held[:, head * width : (head + 1) * width]
            picked.append(
                lax.dot_general(
                    chosen, values, (((0,), (0,)), ((), ())), preferred_element_type=jnp.float32
                )
            )
        scores = jnp.sum(picked[0] * picked[1], axis=1, keepdims=True) * SCORE_SCALE
        top = jnp.max(scores, axis=0, keepdims=True)
        rows = jnp.where(spot == first_head + head, top, rows)
    return rows


def terms_body(*refs, head_count, q_rows, k_rows, shares, width):
    sources, held = refs[:8], refs[-10:]
    xs = refs[8 : 8 + len(shares)]
    ka = refs[8 + len(shares) : 8 + 2 * len(shares)]
    zb = refs[8 + 2 * len(shares) : -10]
    ql, kl, qg, kg, qh, kh, qp, kp, tiles, sems = held
    copies = [
        pltpu.make_async_copy(source, kept, sems.at[n])
        for n, (source, kept) in enumerate(zip(sources, held[:8]))
    ]
    for n in (0, 2, 1, 3, 4, 5, 6, 7):
        copies[n].start()
    device = lax.axis_index("dp")
    for latent, grad, rows, start, n in ((ql, qg, q_rows, 0, 0), (kl, kg, k_rows, q_rows, 1)):
        copies[n].wait()
        copies[n + 2].wait()
        for half in range(2):
            term = jnp.dot(
                latent[half * rows : (half + 1) * rows, :],
                grad[...],
                preferred_element_type=jnp.float32,
            )
            for head in range(head_count):
                tiles[half * head_count + head, start : start + rows, :] = term[
                    :, head * width : (head + 1) * width
                ]
    row_count = q_rows + k_rows
    late = row_count - sum(shares)
    for step in range(2 * head_count):
        tile = tiles[device ^ step]
        outer, inner = step // 2, step % 2
        start = 0
        for out, share in zip(xs if inner else ka, shares):
            out[outer * share : (outer + 1) * share, :] = tile[start : start + share]
            start += share
        zb[outer][inner * late : (inner + 1) * late, :] = tile[start:]
    for copy in copies[4:]:
        copy.wait()
    rows = peak_rows(qh, kh, qp, kp, lax.axis_index("mp") * qp.shape[0])
    xs[0][head_count * shares[0] :, :] = rows
    ka[0][head_count * shares[0] :, :] = rows


def inner_sum_body(ka, rx, *outs):
    count = len(outs)
    share = ka.shape[0] // count // SUB * SUB
    for step, out in enumerate(outs):
        part = slice(step * share, (step + 1) * share)
        out[:share, :] = ka[part, :] + rx[part, :]
        if out.shape[0] > share:
            out[share:, :] = jnp.maximum(ka[count * share :, :], rx[count * share :, :])


def outer_sum_body(*refs):
    *parts, keep, send = refs
    late = keep.shape[0]
    total = parts[0][...]
    for part in parts[1:]:
        total = total + part[...]
    keep[...] = total[:late]
    send[...] = total[late:]


def sum_over_dp(ql, kl, qg, kg, qh, kh, qp, kp, q_rows, k_rows, width):
    count = lax.axis_size("dp")
    head_count = count // 2
    row_count = q_rows + k_rows
    shares = [int(row_count * share) // SUB * SUB for share in FIRST_SHARES]
    extra = [SUB] + [0] * (len(shares) - 1)
    late = row_count - sum(shares)
    body = functools.partial(
        terms_body,
        head_count=head_count,
        q_rows=q_rows,
        k_rows=k_rows,
        shares=shares,
        width=width,
    )
    firsts = [f32(head_count * share + more, width) for share, more in zip(shares, extra)]
    args = (ql, kl, qg, kg, qh, kh, qp, kp)
    made = call(
        body,
        firsts + firsts + [f32(2 * late, width)] * head_count,
        *args,
        scratch=[pltpu.VMEM(arg.shape, arg.dtype) for arg in args]
        + [pltpu.VMEM((count, row_count, width), jnp.float32), pltpu.SemaphoreType.DMA((8,))],
        limit=12,
        fetched=True,
    )
    xs, ka, zb = made[: len(shares)], made[len(shares) : 2 * len(shares)], made[2 * len(shares) :]
    across = [(source, source ^ 1) for source in range(count)]
    steps = list(range(2, head_count)) + [1]

    def along(value, step):
        route = [(source, source ^ (2 * step)) for source in range(count)]
        return lax.ppermute(value, "dp", route)

    rx = [lax.ppermute(value, "dp", across) for value in xs]
    rz = [along(zb[step], step) for step in steps]
    firsts = []
    for n, (share, more) in enumerate(zip(shares, extra)):
        rides = [more if step <= (head_count - 1) // 2 else 0 for step in range(head_count)]
        sums = call(
            inner_sum_body,
            [f32(share + ride, width) for ride in rides],
            ka[n], rx[n],
        )
        firsts.append([sums[0]] + [along(sums[step], step) for step in steps])
    late_keep, late_send = call(outer_sum_body, [f32(late, width)] * 2, zb[0], *rz)
    late_other = lax.ppermute(late_send, "dp", across)
    return [*firsts, [late_keep, late_other]]


def scatter_over_dp(ql, kl, qg, kg, qh, kh, qp, kp, q_rows, k_rows, width):
    count = lax.axis_size("dp")
    head_count = count // 2
    terms = []
    for latent, grad, rows in ((ql, qg, q_rows), (kl, kg, k_rows)):
        term = jnp.dot(latent, grad, preferred_element_type=jnp.float32)
        term = term.reshape(2, rows, head_count, width).transpose(0, 2, 1, 3)
        terms.append(term.reshape(count, rows, width))
    own = lax.psum_scatter(
        jnp.concatenate(terms, axis=1), "dp", scatter_dimension=0, tiled=True
    )[0]

    def body(qh, kh, qp, kp, rows):
        rows[...] = peak_rows(qh, kh, qp, kp, lax.axis_index("mp") * qp.shape[0])

    (rows,) = call(body, [f32(SUB, width)], qh, kh, qp, kp)
    rows = lax.pmax(rows, "dp")
    late = SUB
    return [[jnp.concatenate([own[:-late], rows], axis=0)], [own[-late:]]]


def folded(gram):
    width = gram.shape[0]
    half = width // 2
    line = lax.broadcasted_iota(jnp.int32, (half, width), 0)
    lane = lax.broadcasted_iota(jnp.int32, (half, width), 1)
    low = pltpu.roll(gram[half:, :], half, 1)
    diagonal = jnp.sum(jnp.where(line == lane, low, 0.0), axis=0, keepdims=True)
    return jnp.where((lane < half) & (line > lane), low, gram[:half, :]), diagonal


def unfolded(top, diagonal):
    half, width = top.shape
    line = lax.broadcasted_iota(jnp.int32, (half, width), 0)
    lane = lax.broadcasted_iota(jnp.int32, (half, width), 1)
    turned = jnp.transpose(jnp.concatenate([top, jnp.zeros_like(top)], axis=0))
    over = turned[:half, :]
    low = jnp.where(line > lane, top, jnp.where(line == lane, diagonal, over))
    above = jnp.where((lane < half) & (line > lane), over, top)
    below = jnp.where(lane < half, turned[half:, :], pltpu.roll(low, half, 1))
    return jnp.concatenate([above, below], axis=0)


def gathered(parts):
    top = parts[0].shape[0] - SUB
    total, high = parts[0], parts[0][top:, :]
    for part in parts[1:]:
        total = total + part
        high = jnp.maximum(high, part[top:, :])
    line = lax.broadcasted_iota(jnp.int32, high.shape, 0)
    return jnp.concatenate([total[:top, :], jnp.where(line < 2, total[top:, :], high)], axis=0)


def join_body(pack, given, out):
    out[...] = gathered([pack[...], given[...]])


def total_body(joined, *refs):
    *parts, out = refs
    parts = [part[...] for part in parts]

    @pl.when(lax.axis_index("mp") % 2 == 1)
    def _():
        out[...] = gathered([joined[...], *parts])

    @pl.when(lax.axis_index("mp") % 2 == 0)
    def _():
        if len(parts) > 1:
            out[...] = gathered(parts[:-1])
        else:
            line = lax.broadcasted_iota(jnp.int32, out.shape, 0)
            out[...] = jnp.where(line < out.shape[0] - SUB + 2, 0.0, LOW)


def gram_body(*refs, groups, q_rows):
    mq, mk = refs[0], refs[1]
    mq_new, mk_new, pack = refs[-3:]
    own, start = [], 2
    for n, size in enumerate(groups):
        parts = refs[start : start + size]
        start += size
        share = parts[0].shape[0] - (0 if n else SUB)
        total = parts[0][:share, :]
        for part in parts[1:]:
            total = total + part[:share, :]
        own.append(total)
        if not n:
            rows = parts[0][share:, :]
            for part in parts[1:]:
                if part.shape[0] > share:
                    rows = jnp.maximum(rows, part[share:, :])
    own = jnp.concatenate(own, axis=0)
    q = MOMENTUM * mq[...] + own[:q_rows]
    k = MOMENTUM * mk[...] + own[q_rows:]
    mq_new[...] = q
    mk_new[...] = k
    q_gram = own_gram(q)
    k_gram = own_gram(k)
    half = q_gram.shape[0] // 2
    pack[:half, :], q_rest = folded(q_gram)
    pack[half : 2 * half, :], k_rest = folded(k_gram)
    line = lax.broadcasted_iota(jnp.int32, rows.shape, 0)
    pack[2 * half :, :] = jnp.where(line == 0, q_rest, jnp.where(line == 1, k_rest, rows))


def finish_body(*refs, head_count, norms):
    total, other, mq, mk, wq, wk = refs[:6]
    wq_new, wk_new, mq_out, mk_out, sems = refs[6:]
    copies = [
        pltpu.make_async_copy(mq, mq_out, sems.at[0]),
        pltpu.make_async_copy(mk, mk_out, sems.at[1]),
    ]
    for copy in copies:
        copy.start()
    merged = gathered([total[...], other[...]])
    width = total.shape[1]
    half = width // 2
    rows = merged[2 * half :, :]
    spot = lax.broadcasted_iota(jnp.int32, rows.shape, 1)
    line = lax.broadcasted_iota(jnp.int32, rows.shape, 0)
    own = lax.axis_index("dp") % head_count
    peak = jnp.max(
        jnp.where((spot == own) & (line > 1), rows, LOW), axis=(0, 1), keepdims=True
    )
    shrink = jnp.sqrt(CLIP_LEVEL / jnp.maximum(peak, CLIP_LEVEL))
    grams = [
        unfolded(merged[n * half : (n + 1) * half, :], rows[n : n + 1, :]) for n in range(2)
    ]
    line = lax.broadcasted_iota(jnp.int32, (width, width), 0)
    diagonal = line == lax.broadcasted_iota(jnp.int32, (width, width), 1)
    unit = jnp.where(diagonal, COEFF_A, 0.0)
    moved = [left(pieces(value[...])) for value in (mq, mk)]
    scales, shrunk = [], []
    for gram in grams:
        trace = jnp.sum(jnp.where(diagonal, gram, 0.0), axis=(0, 1), keepdims=True)
        scales.append(1.0 / jnp.sqrt(trace + 1.0))
        shrunk.append(scales[-1] * scales[-1])
    both = range(2)
    for step in range(ITERS):
        factors = [1.0, 1.0] if step else shrunk
        parts = [pieces(gram) for gram in grams]
        bases = [right(part) for part in parts]
        if step and step + 1 == ITERS:
            inner = [stacked(moved[n], bases[n]) for n in both]
            outer = [left(pieces(COEFF_B * held[n] + COEFF_C * inner[n])) for n in both]
            held = [COEFF_A * held[n] + stacked(outer[n], bases[n]) for n in both]
            break
        squares = [stacked(left(parts[n]), bases[n]) for n in both]
        splits = [
            pieces(
                unit
                + factors[n] * (COEFF_B * grams[n] + (COEFF_C * factors[n]) * squares[n])
            )
            for n in both
        ]
        follows = [right(split) for split in splits]
        if step + 1 < ITERS:
            inner = [stacked(left(splits[n]), bases[n]) * factors[n] for n in both]
            grams = [stacked(left(pieces(inner[n])), follows[n]) for n in both]
        held = [stacked(moved[n], follows[n]) for n in both]
        moved = [left(pieces(value)) for value in held]
    keep = 1.0 - STEP_SIZE * DECAY
    for n, (weight, out) in enumerate(((wq, wq_new), (wk, wk_new))):
        out[...] = (weight[...] * keep - (norms[n] * scales[n]) * held[n]) * shrink
    for copy in copies:
        copy.wait()


def local(
    q_latent,
    kv_latent,
    q_head_grad,
    k_head_grad,
    q_heads,
    k_heads,
    query_pick,
    key_pick,
    q_weight,
    k_weight,
    q_moment,
    k_moment,
):
    dp, mp = lax.axis_size("dp"), lax.axis_size("mp")
    head_count = dp // 2
    tokens = q_latent.shape[0]
    q_rows, k_rows = q_latent.shape[2], kv_latent.shape[2]
    width = q_moment.shape[2]
    ql = jnp.transpose(q_latent, (1, 2, 0)).reshape(2 * q_rows, tokens)
    kl = jnp.transpose(kv_latent, (1, 2, 0)).reshape(2 * k_rows, tokens)
    qp = jnp.transpose(query_pick[0], (1, 0))
    kp = jnp.transpose(key_pick[0], (1, 0))
    direct = dp <= 16 and dp & (dp - 1) == 0
    reduce = sum_over_dp if direct else scatter_over_dp
    groups = reduce(
        ql, kl, q_head_grad, k_head_grad, q_heads, k_heads, qp, kp, q_rows, k_rows, width
    )
    folded_pair = f32(width + SUB, width)
    mq, mk, pack = call(
        functools.partial(gram_body, groups=[len(group) for group in groups], q_rows=q_rows),
        [f32(q_rows, width), f32(k_rows, width), folded_pair],
        q_moment[0], k_moment[0], *sum(groups, []),
    )
    pair = [(core, core ^ 1) for core in range(mp)]
    given = lax.ppermute(pack, "mp", pair)
    (joined,) = call(join_body, [folded_pair], pack, given)
    peers = [(1, near) for near in reversed(range(mp // 2))]
    peers += [(0, near) for near in range(1, mp // 2)]
    parts = []
    for n in range(mp // 2):
        shifts = [peers[2 * n + 1] if 2 * n + 1 < len(peers) else (0, 0), peers[2 * n]]
        route = []
        for d in range(dp):
            for m in range(mp):
                far, near = shifts[m % 2]
                route.append(
                    (d * mp + m, (d + far * head_count) % dp * mp + (m + 2 * near) % mp)
                )
        parts.append(lax.ppermute(joined, ("dp", "mp"), route))
    (total,) = call(total_body, [folded_pair], joined, *parts)
    back = lax.ppermute(total, "mp", pair)
    norms = [STEP_SIZE * 0.2 * math.sqrt(2 * rows * mp) for rows in (q_rows, k_rows)]
    wq_new, wk_new, mq_new, mk_new = call(
        functools.partial(finish_body, head_count=head_count, norms=norms),
        [f32(q_rows, width), f32(k_rows, width)]
        + [pltpu.HBM(value.shape, jnp.float32) for value in (mq, mk)],
        total, back, mq, mk, q_weight[0], k_weight[0],
        scratch=[pltpu.SemaphoreType.DMA((2,))],
    )
    return (wq_new[None], wk_new[None], mq_new[None], mk_new[None])


def solution(mesh):
    in_specs = (
        P("dp", None, "mp"),
        P("dp", None, "mp"),
        P("dp", None),
        P("dp", None),
        P("dp", "mp"),
        P("dp", "mp"),
        P("dp", None, "mp"),
        P("dp", None, "mp"),
        P("dp", "mp", None),
        P("dp", "mp", None),
        P("dp", "mp", None),
        P("dp", "mp", None),
    )
    out_specs = (P("dp", "mp", None), P("dp", "mp", None), P("dp", "mp", None), P("dp", "mp", None))

    return jax.shard_map(local, mesh=mesh, in_specs=in_specs, out_specs=out_specs, check_vma=False)
```
